32 devices in a mesh: grp: 2 (over x), page: 16 (over z, y, core).
Axes of the slice: x: 2, y: 2, z: 4, core: 2. Of those that a mesh axis runs over, the one named last changes fastest.
Arguments:
- queries: bfloat16 [32, 32, 128], P(('grp', 'page')), may hold values from -2 to 2
- patches: bfloat16 [65536, 128], P(('grp', 'page')), may hold values from -2 to 2
- page_blocks: int32 [512, 2], P(('grp', 'page')), may hold values from -1 to 63, as said below
- lengths: int32 [64], replicated, may hold values from 2 to 4352, as said below
- labels: int32 [32, 64], replicated, may hold values 0 or 1
Outputs:
- patch_grad: float32 [65536, 128], P(('grp', 'page'))
- query_grad: float32 [32, 32, 128], P(('grp', 'page'))
- mean_loss: float32 [1], replicated
The draws below stay inside these ranges and needn't reach their ends.
Inputs may be any that keep to these rules, and one draw needn't show every extreme that they name: `page_blocks`: row i describes block slot i (patch rows i * 128 to (i + 1) * 128 - 1): its page and which of that page's blocks it is, counting from 0, or -1 and 0 for an empty slot. On each device the live slots come first among its 16 slots; every device has 2 or more live slots, and in every group some device has all 16 live. Page p has ceil(lengths[p] / 128) blocks in consecutive live slots in order, which may continue over consecutive devices of the page axis; the pages of one grp index form a contiguous range of ids, lie only on that index's devices and appear in increasing order. `lengths`: A page's last block holds 2 to 128 of its patches.
All inputs are finite; a program needn't handle non-finite values.
Results may differ from the reference program's by a relative error of at most 0.0017.
Values may be sent and summed in bfloat16 or wider, within the bound.
No kernel may reach another device: no remote copies, remote signals or barrier semaphores. Data moves between devices by JAX's collectives and lax.ppermute only.
A program may use at most 64 MiB of HBM per device.

```python
import jax
import jax.numpy as jnp
from jax import lax

D = 128
QUESTION_WORDS = 32
BROWS = 128
PAGE_DEV = 2
BLK_DEV = 16
QUESTION_NUMBER = 32
DOCUMENT_NUMBER = 64
BLOCKS = 512
N_GRP = 2
N_PAGE = 16


def group_layout(key):
    slot_total = BLK_DEV * N_PAGE
    group_pages = PAGE_DEV * N_PAGE
    middle = N_PAGE // 2
    cap_key, full_key, cut_key, rem_key = jax.random.split(key, 4)
    capacity = jax.random.randint(cap_key, (N_PAGE,), PAGE_DEV, BLK_DEV + 1)
    busiest = jax.random.randint(full_key, (), 0, N_PAGE)
    device_ids = jnp.arange(N_PAGE)
    capacity = jnp.where(device_ids == busiest, BLK_DEV, capacity)
    capacity = jnp.where((device_ids >= middle - 3) & (device_ids <= middle + 2), BLK_DEV, capacity)
    capacity = jnp.where((device_ids <= 1) | (device_ids >= N_PAGE - 2), BLK_DEV, capacity)
    used_slots = jnp.sum(capacity)
    cap_start = jnp.cumsum(capacity) - capacity
    span_start = cap_start[middle - 1] - 1
    span_end = cap_start[middle + 1] + 1
    candidates = jnp.arange(1, slot_total, dtype=jnp.int32)
    random_bits = jax.random.randint(cut_key, (slot_total - 1,), 0, 16384)
    inside = (candidates > span_start) & (candidates < span_end)
    barred = (candidates == cap_start[1]) | (candidates == cap_start[N_PAGE - 1])
    allowed = (candidates < used_slots) & jnp.logical_not(inside) & jnp.logical_not(barred)
    device_edge = jnp.any(candidates[:, None] == cap_start[None, :], axis=1)
    forced = ((candidates == span_start) | (candidates == span_end) | device_edge) & allowed
    priority = random_bits * slot_total + candidates + jnp.where(allowed, 1 << 30, 0) + jnp.where(forced, 1 << 29, 0)
    cut_points = jnp.sort(lax.top_k(priority, group_pages - 1)[1].astype(jnp.int32) + 1)
    starts = jnp.concatenate([jnp.zeros((1,), jnp.int32), cut_points])
    page_ends = jnp.concatenate([cut_points, used_slots.reshape(1).astype(jnp.int32)])
    counts = page_ends - starts
    remainder = jax.random.randint(rem_key, (group_pages,), 2, BROWS + 1)
    remainder = jnp.where(counts == jnp.max(counts), BROWS, remainder)
    lengths = (counts - 1) * BROWS + remainder
    slot_device = jnp.arange(slot_total) // BLK_DEV
    slot_within = jnp.arange(slot_total) % BLK_DEV
    occupied = slot_within < capacity[slot_device]
    position = cap_start[slot_device] + slot_within
    page_local = jnp.sum((starts[None, :] <= position[:, None]).astype(jnp.int32), axis=1) - 1
    number = position - starts[page_local]
    return (lengths, occupied, page_local, number)


def full_layout(key):
    base_key = jax.random.fold_in(key, 7001)

    def one_group(group_index):
        lengths, occupied, page_local, number = group_layout(jax.random.fold_in(base_key, group_index))
        page_global = jnp.where(occupied, page_local + group_index * PAGE_DEV * N_PAGE, -1)
        number = jnp.where(occupied, number, 0)
        return (lengths, jnp.stack([page_global, number], axis=1))
    lengths, blocks = jax.vmap(one_group)(jnp.arange(N_GRP, dtype=jnp.int32))
    return (lengths.reshape(-1).astype(jnp.int32), blocks.reshape(-1, 2).astype(jnp.int32))


def draw_page_blocks(key, part):
    return full_layout(key)[1]


def draw_lengths(key, part):
    return full_layout(key)[0]


def draw_patches(key, part):
    base_key = jax.random.fold_in(key, 4001)
    values = jnp.clip(jax.random.normal(base_key, (BLOCKS * BROWS, D), jnp.float32), -6.0, 6.0) * D ** (-0.5)
    return values.astype(jnp.bfloat16)


def draw_queries(key, part):
    base_key = jax.random.fold_in(key, 5001)
    values = jnp.clip(jax.random.normal(base_key, (QUESTION_NUMBER, QUESTION_WORDS, D), jnp.float32), -6.0, 6.0) * D ** (-0.5)
    return values.astype(jnp.bfloat16)


def plant(drawn, rng, low, top_value):
    index_at = [jax.random.randint(jax.random.fold_in(rng, axis), (), 0, length) for axis, length in enumerate(drawn.shape)]
    main_axis = drawn.shape.index(max(drawn.shape))
    next_to = index_at[:main_axis] + [(index_at[main_axis] + 1) % drawn.shape[main_axis]] + index_at[main_axis + 1:]
    return drawn.at[tuple(index_at)].set(low).at[tuple(next_to)].set(top_value)


def setup_inputs(seed: int = 0) -> dict:
    key_list = jax.random.split(jax.random.key(seed), 6)
    queries = draw_queries(jax.random.fold_in(key_list[5], 71), 0)
    patches = draw_patches(jax.random.fold_in(key_list[5], 71), 0)
    page_blocks = draw_page_blocks(jax.random.fold_in(key_list[5], 71), 0)
    lengths = draw_lengths(jax.random.fold_in(key_list[5], 71), 0)
    labels = plant((jax.random.randint(key_list[4], (QUESTION_NUMBER, DOCUMENT_NUMBER), 0, 8) < 1).astype(jnp.int32), jax.random.fold_in(key_list[4], 1), 0, 1)
    return {"queries": queries, "patches": patches, "page_blocks": page_blocks, "lengths": lengths, "labels": labels}


smoothing_divisor = 0.05
logit_scale = 10.0
logit_bias = -4.0
very_low = -1e30


def rows_alive(page_blocks, lengths):
    slot_pages = page_blocks[:, 0]
    numbers = page_blocks[:, 1]
    safe_pages = jnp.where(slot_pages < 0, 0, slot_pages).astype(jnp.int32)
    page_length = lengths[safe_pages]
    offsets = numbers[:, None] * BROWS + jnp.arange(BROWS, dtype=jnp.int32)[None, :]
    return (slot_pages[:, None] >= 0) & (offsets < page_length[:, None])


def reference(queries, patches, page_blocks, lengths, labels):
    question_word_vectors = queries.reshape(QUESTION_NUMBER * QUESTION_WORDS, D)
    patch_blocks = patches.reshape(BLOCKS, BROWS, D)
    live_rows = rows_alive(page_blocks, lengths)
    slot_pages = page_blocks[:, 0]
    segment_ids = jnp.where(slot_pages < 0, DOCUMENT_NUMBER, slot_pages).astype(jnp.int32)
    safe_pages = jnp.where(slot_pages < 0, 0, slot_pages).astype(jnp.int32)

    def block_stats(operands):
        image_region_group, live_mask = operands
        tempered_similarity = jnp.dot(question_word_vectors, image_region_group.T, preferred_element_type=jnp.float32) * (1.0 / smoothing_divisor)
        tempered_similarity = jnp.where(live_mask[None, :], tempered_similarity, very_low)
        peak_row = jnp.max(tempered_similarity, axis=1)
        mass_row = jnp.sum(jnp.where(live_mask[None, :], jnp.exp(tempered_similarity - peak_row[:, None]), 0.0), axis=1)
        return peak_row, mass_row

    block_peak, block_mass = lax.map(block_stats, (patch_blocks, live_rows))
    page_peak = jax.ops.segment_max(block_peak, segment_ids, num_segments=DOCUMENT_NUMBER + 1)
    rescaled = block_mass * jnp.exp(block_peak - page_peak[segment_ids])
    page_mass = jax.ops.segment_sum(rescaled, segment_ids, num_segments=DOCUMENT_NUMBER + 1)
    document_smooth_maximum = page_peak[:DOCUMENT_NUMBER] + jnp.log(page_mass[:DOCUMENT_NUMBER])
    similarity_values = smoothing_divisor * jnp.sum(document_smooth_maximum.reshape(DOCUMENT_NUMBER, QUESTION_NUMBER, QUESTION_WORDS), axis=2).T
    logits = logit_scale / QUESTION_WORDS * similarity_values + logit_bias
    label_signs = 2.0 * labels.astype(jnp.float32) - 1.0
    mean_loss = jnp.sum(jax.nn.softplus(-label_signs * logits)) / QUESTION_NUMBER
    logit_grad = -label_signs * jax.nn.sigmoid(-label_signs * logits)

    def block_grads(query_grad, operands):
        image_region_group, live_mask, slot_page = operands
        tempered_similarity = jnp.dot(question_word_vectors, image_region_group.T, preferred_element_type=jnp.float32) * (1.0 / smoothing_divisor)
        row_lse = document_smooth_maximum[slot_page]
        weights = jnp.where(live_mask[None, :], jnp.exp(tempered_similarity - row_lse[:, None]), 0.0)
        row_grad = jnp.repeat(logit_grad[:, slot_page], QUESTION_WORDS) * (logit_scale / QUESTION_WORDS)
        coupling = (row_grad[:, None] * weights).astype(jnp.bfloat16)
        block_grad = jnp.dot(coupling.T, question_word_vectors, preferred_element_type=jnp.float32)
        query_grad = query_grad + jnp.dot(coupling, image_region_group, preferred_element_type=jnp.float32)
        return query_grad, block_grad

    query_grad, patch_grads = lax.scan(block_grads, jnp.zeros((QUESTION_NUMBER * QUESTION_WORDS, D), jnp.float32), (patch_blocks, live_rows, safe_pages))
    return patch_grads.reshape(BLOCKS * BROWS, D), query_grad.reshape(QUESTION_NUMBER, QUESTION_WORDS, D), jnp.reshape(mean_loss, (1,))
```

```python
import jax
import jax.numpy as jnp
from jax import lax
from jax.experimental import pallas as pl
from jax.experimental.pallas import tpu as pltpu
from jax.sharding import PartitionSpec as P

QUESTION_WORDS = 32
BROWS = 128

smoothing_divisor = 0.05
logit_scale = 10.0
logit_bias = -4.0
very_low = -1e30
LOG2E = 1.4426950408889634
LN2 = 0.6931471805599453
SCALE2 = LOG2E / smoothing_divisor
CHUNK = 256
LOSS_ROWS = 8

f32 = jnp.float32
bf16 = jnp.bfloat16
VMEM = pl.BlockSpec(memory_space=pltpu.VMEM)
SMEM = pl.BlockSpec(memory_space=pltpu.SMEM)


def live_of_slot(pb_ref, len_ref, slot):
    page = pb_ref[slot, 0]
    length = len_ref[jnp.maximum(page, 0)]
    return jnp.where(page < 0, 0, length - pb_ref[slot, 1] * BROWS)


def lse_rows(values, mask):
    peak = jnp.max(jnp.where(mask, values, very_low), axis=0, keepdims=True)
    mass = jnp.sum(jnp.where(mask, jnp.exp2(values - peak), 0.0), axis=0, keepdims=True)
    return peak + jnp.log2(mass)


def scored(q_ref, p_ref, live, slot, lo):
    block = p_ref[pl.ds(pl.multiple_of(slot * BROWS, BROWS), BROWS), :]
    z = lax.dot_general(
        block, q_ref[lo : lo + CHUNK, :], (((1,), (1,)), ((), ())), preferred_element_type=f32
    )
    rows = lax.broadcasted_iota(jnp.int32, (BROWS, 1), 0)
    return jnp.where(rows < live, z * SCALE2, very_low)


def stats_kernel(pb_ref, len_ref, pbv_ref, q_ref, p_ref, lse_ref, send_ref):
    slots, rows = lse_ref.shape

    def one(slot, carry):
        live = live_of_slot(pb_ref, len_ref, slot)
        for lo in range(0, rows, CHUNK):
            z = scored(q_ref, p_ref, live, slot, lo)
            peak = jnp.max(z, axis=0, keepdims=True)
            mass = jnp.sum(jnp.exp2(z - peak), axis=0, keepdims=True)
            lse_ref[pl.ds(slot, 1), lo : lo + CHUNK] = peak + jnp.log2(mass)
        return carry

    lax.fori_loop(0, slots, one, 0)
    pages = pbv_ref[:, 0:1]
    first = pb_ref[0, 0]
    last = jnp.max(pages)
    values = lse_ref[...]
    head = lse_rows(values, pages == first)
    tail = lse_rows(values, pages == last)
    mine = lax.axis_index("page")
    peers = send_ref.shape[0]
    for peer in range(peers):
        up = peer > mine
        send_ref[peer, :, :rows] = jnp.where(up, tail, head)
        send_ref[peer, :, rows:] = jnp.full((1, 128), jnp.where(up, last, first).astype(f32))


def merge_kernel(pb_ref, pbv_ref, lab_ref, lse_ref, page_ref, sign_ref):
    slots, rows = lse_ref.shape
    pages = pbv_ref[:, 0:1]
    values = lse_ref[...]
    for slot in range(slots):
        page_ref[slot : slot + 1, :] = lse_rows(values, pages == pb_ref[slot, 0])
    queries, page_count = lab_ref.shape
    ids = lax.broadcasted_iota(jnp.int32, (slots, page_count), 1)
    picked = lax.dot_general(
        (ids == pages).astype(bf16),
        lab_ref[...].astype(bf16),
        (((1,), (1,)), ((), ())),
        preferred_element_type=f32,
    )
    spread = (
        lax.broadcasted_iota(jnp.int32, (queries, rows), 1) // QUESTION_WORDS
        == lax.broadcasted_iota(jnp.int32, (queries, rows), 0)
    ).astype(bf16)
    sign_ref[...] = 2.0 * jnp.dot(picked.astype(bf16), spread, preferred_element_type=f32) - 1.0


def add_lse(one, two):
    peak = jnp.maximum(one, two)
    return peak + jnp.log2(jnp.exp2(one - peak) + jnp.exp2(two - peak))


def three_terms(value):
    high = value.astype(bf16)
    rest = value - high.astype(f32)
    mid = rest.astype(bf16)
    return high, mid, (rest - mid.astype(f32)).astype(bf16)


def query_kernel(
    pb_ref, len_ref, pbv_ref, page_ref, sign_ref, recv_ref, q_ref, p_ref, out_ref, lse_ref, row_ref,
    acc_ref,
):
    slots, rows = page_ref.shape
    peers = recv_ref.shape[0]
    mine = lax.axis_index("page")
    pages = pbv_ref[:, 0:1]
    first = pb_ref[0, 0]
    last = jnp.max(pages)

    def gathered(wanted, below):
        peak = jnp.full((1, rows), very_low, f32)
        parts = []
        for peer in range(peers):
            side = peer < mine if below else peer > mine
            same = (recv_ref[peer, :, rows : rows + 1] == wanted.astype(f32)) & side
            parts.append(jnp.where(same, recv_ref[peer, :, :rows], very_low))
            peak = jnp.maximum(peak, parts[-1])
        mass = jnp.zeros((1, rows), f32)
        for part in parts:
            mass = mass + jnp.where(part > 0.5 * very_low, jnp.exp2(part - peak), 0.0)
        return peak + jnp.log2(jnp.maximum(mass, 1e-30))

    value = page_ref[...]
    value = jnp.where(pages == first, add_lse(value, gathered(first, True)), value)
    value = jnp.where(pages == last, add_lse(value, gathered(last, False)), value)
    value = jnp.where(pages >= 0, value, 0.0)
    lse_ref[...] = value
    same_group = (
        lax.broadcasted_iota(jnp.int32, (CHUNK, CHUNK), 0) // QUESTION_WORDS
        == lax.broadcasted_iota(jnp.int32, (CHUNK, CHUNK), 1) // QUESTION_WORDS
    ).astype(bf16)
    counted = (pages >= 0) & (pbv_ref[:, 1:2] == 0)
    loss = jnp.zeros((), f32)
    for lo in range(0, rows, CHUNK):
        piece = jnp.concatenate(three_terms(value[:, lo : lo + CHUNK]), axis=0)
        total = jnp.dot(piece, same_group, preferred_element_type=f32)
        total = total[:slots] + total[slots : 2 * slots] + total[2 * slots :]
        scores = (smoothing_divisor * LN2) * total
        logits = (logit_scale / QUESTION_WORDS) * scores + logit_bias
        sign = sign_ref[:, lo : lo + CHUNK]
        margin = -sign * logits
        small = jnp.exp(-jnp.abs(margin))
        pair = jnp.maximum(margin, 0.0) + jnp.log1p(small)
        loss = loss + jnp.sum(jnp.where(counted, pair, 0.0))
        sigmoid = jnp.where(margin >= 0.0, 1.0, small) / (1.0 + small)
        row_ref[:, lo : lo + CHUNK] = -sign * sigmoid * (logit_scale / QUESTION_WORDS)
    loss = loss * (1.0 / QUESTION_WORDS)

    acc_ref[...] = jnp.zeros_like(acc_ref)

    def one(slot, carry):
        live = live_of_slot(pb_ref, len_ref, slot)
        block = p_ref[pl.ds(pl.multiple_of(slot * BROWS, BROWS), BROWS), :]
        for lo in range(0, rows, CHUNK):
            coupling = coupled(q_ref, p_ref, lse_ref, row_ref, live, slot, lo)
            acc_ref[:, lo : lo + CHUNK] += lax.dot_general(
                block, coupling, (((0,), (0,)), ((), ())), preferred_element_type=f32
            )
        return carry

    lax.fori_loop(0, slots, one, 0)
    devices = out_ref.shape[0]
    local = rows // devices
    out_ref[:, :local, :] = acc_ref[...].T.astype(bf16).reshape(devices, local, BROWS)
    terms = three_terms(jnp.full((1, BROWS), loss))
    tail = jnp.concatenate([t.astype(f32) for t in terms] + [jnp.zeros((LOSS_ROWS - 3, BROWS), f32)], axis=0)
    for device in range(devices):
        out_ref[device, local:, :] = tail.astype(bf16)


def coupled(q_ref, p_ref, lse_ref, row_ref, live, slot, lo):
    z = scored(q_ref, p_ref, live, slot, lo)
    weights = jnp.exp2(z - lse_ref[pl.ds(slot, 1), lo : lo + CHUNK])
    return (row_ref[pl.ds(slot, 1), lo : lo + CHUNK] * weights).astype(bf16)


def patch_kernel(pb_ref, len_ref, lse_ref, row_ref, q_ref, p_ref, out_ref):
    slots, rows = lse_ref.shape

    def one(slot, carry):
        live = live_of_slot(pb_ref, len_ref, slot)
        total = jnp.zeros((BROWS, BROWS), f32)
        for lo in range(0, rows, CHUNK):
            coupling = coupled(q_ref, p_ref, lse_ref, row_ref, live, slot, lo)
            total = total + jnp.dot(
                coupling, q_ref[lo : lo + CHUNK, :], preferred_element_type=f32
            )
        out_ref[pl.ds(pl.multiple_of(slot * BROWS, BROWS), BROWS), :] = total
        return carry

    lax.fori_loop(0, slots, one, 0)


def final_kernel(scale, recv_ref, grad_ref, loss_ref):
    devices, padded, _ = recv_ref.shape
    total = jnp.zeros((padded, BROWS), f32)
    for device in range(devices):
        total = total + recv_ref[device].astype(f32)
    local = padded - LOSS_ROWS
    grad_ref[...] = total[:local]
    loss_ref[...] = (total[local : local + 1] + total[local + 1 : local + 2] + total[local + 2 : local + 3]) * scale


def cost(flops, bytes_accessed=0, transcendentals=0):
    return pl.CostEstimate(
        flops=flops, bytes_accessed=bytes_accessed, transcendentals=transcendentals
    )


def shards(queries, patches, page_blocks, lengths, labels):
    axes = ("grp", "page")
    devices = lax.axis_size(axes)
    peers = lax.axis_size("page")
    slots = page_blocks.shape[0]
    width = patches.shape[1]
    local_rows = queries.reshape(-1, width)
    local = local_rows.shape[0]
    rows = local * devices
    matmul = 2 * rows * patches.shape[0] * width
    q = lax.all_to_all(
        jnp.broadcast_to(local_rows[None], (devices, local, width)), axes, 0, 0, tiled=True
    ).reshape(rows, width)

    lse, send = pl.pallas_call(
        stats_kernel,
        in_specs=[SMEM, SMEM, VMEM, VMEM, VMEM],
        out_specs=[VMEM, VMEM],
        out_shape=[
            jax.ShapeDtypeStruct((slots, rows), f32),
            jax.ShapeDtypeStruct((peers, 1, rows + 128), f32),
        ],
        cost_estimate=cost(matmul),
        name="stats",
    )(page_blocks, lengths, page_blocks, q, patches)
    recv = lax.all_to_all(send, "page", 0, 0, tiled=True)

    page_lse, sign = pl.pallas_call(
        merge_kernel,
        in_specs=[SMEM, VMEM, VMEM, VMEM],
        out_specs=[VMEM, VMEM],
        out_shape=[
            jax.ShapeDtypeStruct((slots, rows), f32),
            jax.ShapeDtypeStruct((slots, rows), f32),
        ],
        cost_estimate=cost(matmul),
        name="merge",
    )(page_blocks, page_blocks, labels, lse)

    parts, full_lse, row_grad = pl.pallas_call(
        query_kernel,
        in_specs=[SMEM, SMEM, VMEM, VMEM, VMEM, VMEM, VMEM, VMEM],
        out_specs=[VMEM, VMEM, VMEM],
        out_shape=[
            jax.ShapeDtypeStruct((devices, local + LOSS_ROWS, width), bf16),
            jax.ShapeDtypeStruct((slots, rows), f32),
            jax.ShapeDtypeStruct((slots, rows), f32),
        ],
        scratch_shapes=[pltpu.VMEM((width, rows), f32)],
        cost_estimate=cost(2 * matmul),
        name="query",
    )(page_blocks, lengths, page_blocks, page_lse, sign, recv, q, patches)
    gathered = lax.all_to_all(parts, axes, 0, 0, tiled=True)

    patch_grad = pl.pallas_call(
        patch_kernel,
        in_specs=[SMEM, SMEM, VMEM, VMEM, VMEM, VMEM],
        out_specs=VMEM,
        out_shape=jax.ShapeDtypeStruct(patches.shape, f32),
        cost_estimate=cost(2 * matmul),
        name="patch",
    )(page_blocks, lengths, full_lse, row_grad, q, patches)

    query_grad, loss = pl.pallas_call(
        lambda *refs: final_kernel(QUESTION_WORDS / rows, *refs),
        in_specs=[VMEM],
        out_specs=[VMEM, VMEM],
        out_shape=[
            jax.ShapeDtypeStruct((local, width), f32),
            jax.ShapeDtypeStruct((1, BROWS), f32),
        ],
        cost_estimate=cost(devices * local * width),
        name="final",
    )(gathered)
    return (patch_grad, query_grad.reshape(queries.shape), loss[0, :1])


def solution(mesh):
    placed = (
        P(("grp", "page"), None, None),
        P(("grp", "page"), None),
        P(("grp", "page"), None),
        P(),
        P(),
    )
    return jax.shard_map(
        shards,
        mesh=mesh,
        in_specs=placed,
        out_specs=(P(("grp", "page"), None), P(("grp", "page"), None, None), P()),
        check_vma=False,
    )
```

```python
import jax
import jax.numpy as jnp
from jax import lax
from jax.experimental import pallas as pl
from jax.experimental.pallas import tpu as pltpu
from jax.sharding import PartitionSpec as P

QUESTION_WORDS = 32
BROWS = 128

smoothing_divisor = 0.05
logit_scale = 10.0
logit_bias = -4.0
very_low = -1e30
LOG2E = 1.4426950408889634
LN2 = 0.6931471805599453
SCALE2 = LOG2E / smoothing_divisor
CHUNK = 256
LOSS_ROWS = 8
INSIDE, HEAD, TAIL = 0, 1, 2

f32 = jnp.float32
bf16 = jnp.bfloat16
VMEM = pl.BlockSpec(memory_space=pltpu.VMEM)
SMEM = pl.BlockSpec(memory_space=pltpu.SMEM)


def lse_rows(values, mask):
    peak = jnp.max(jnp.where(mask, values, very_low), axis=0, keepdims=True)
    mass = jnp.sum(jnp.where(mask, jnp.exp2(values - peak), 0.0), axis=0, keepdims=True)
    return peak + jnp.log2(mass)


def add_lse(one, two):
    peak = jnp.maximum(one, two)
    return peak + jnp.log2(jnp.exp2(one - peak) + jnp.exp2(two - peak))


def chosen_row(values, mask):
    return jnp.max(jnp.where(mask, values, very_low), axis=0, keepdims=True)


def three_terms(value):
    high = value.astype(bf16)
    rest = value - high.astype(f32)
    mid = rest.astype(bf16)
    return high, mid, (rest - mid.astype(f32)).astype(bf16)


def block_of(p_ref, slot):
    return p_ref[pl.ds(pl.multiple_of(slot * BROWS, BROWS), BROWS), :]


def scored(qt_ref, block, live_ref, slot, lo):
    z = jnp.dot(block, qt_ref[:, lo : lo + CHUNK], preferred_element_type=f32)
    rows = lax.broadcasted_iota(jnp.int32, (BROWS, 1), 0)
    return jnp.where(rows < live_ref[pl.ds(slot, 1), 0:1], z * SCALE2, very_low)


def prep_kernel(pb_ref, len_ref, lab_ref, live_ref, sign_ref):
    slots, rows = sign_ref.shape
    queries, page_count = lab_ref.shape
    pages = pb_ref[:, 0:1]
    ids = lax.broadcasted_iota(jnp.int32, (slots, page_count), 1)
    hit = ids == pages
    length = jnp.sum(jnp.where(hit, len_ref[...], 0).astype(f32), axis=1, keepdims=True)
    live = length.astype(jnp.int32) - pb_ref[:, 1:2] * BROWS
    live_ref[...] = jnp.broadcast_to(jnp.where(pages < 0, 0, live), live_ref.shape)
    picked = lax.dot_general(
        hit.astype(bf16),
        lab_ref[...].astype(bf16),
        (((1,), (1,)), ((), ())),
        preferred_element_type=f32,
    )
    spread = (
        lax.broadcasted_iota(jnp.int32, (queries, rows), 1) // QUESTION_WORDS
        == lax.broadcasted_iota(jnp.int32, (queries, rows), 0)
    ).astype(bf16)
    sign_ref[...] = 2.0 * jnp.dot(picked.astype(bf16), spread, preferred_element_type=f32) - 1.0


def stats_kernel(pb_ref, live_ref, q_ref, p_ref, lse_ref, send_ref, qt_ref):
    slots, rows = lse_ref.shape
    qt_ref[...] = q_ref[...].T
    for slot in range(slots):
        block = block_of(p_ref, slot)
        for lo in range(0, rows, CHUNK):
            z = scored(qt_ref, block, live_ref, slot, lo)
            peak = jnp.max(z, axis=0, keepdims=True)
            mass = jnp.sum(jnp.exp2(z - peak), axis=0, keepdims=True)
            lse_ref[pl.ds(slot, 1), lo : lo + CHUNK] = peak + jnp.log2(mass)
    pages = pb_ref[:, 0:1]
    first = pages[0:1]
    last = jnp.max(pages, axis=0, keepdims=True)
    values = lse_ref[...]
    head = lse_rows(values, pages == first)
    tail = lse_rows(values, pages == last)
    mine = lax.axis_index("page")
    for peer in range(send_ref.shape[0]):
        up = peer > mine
        send_ref[peer, :, :rows] = jnp.where(up, tail, head)
        send_ref[peer, :, rows:] = jnp.broadcast_to(jnp.where(up, last, first).astype(f32), (1, 128))


def gradients(value, sign):
    count, rows = value.shape
    same_group = (
        lax.broadcasted_iota(jnp.int32, (CHUNK, CHUNK), 0) // QUESTION_WORDS
        == lax.broadcasted_iota(jnp.int32, (CHUNK, CHUNK), 1) // QUESTION_WORDS
    ).astype(bf16)
    totals = []
    for lo in range(0, rows, CHUNK):
        total = [
            jnp.dot(term, same_group, preferred_element_type=f32)
            for term in three_terms(value[:, lo : lo + CHUNK])
        ]
        totals.append(total[0] + total[1] + total[2])
    scores = (smoothing_divisor * LN2) * jnp.concatenate(totals, axis=1)
    logits = (logit_scale / QUESTION_WORDS) * scores + logit_bias
    margin = -sign * logits
    small = jnp.exp(-jnp.abs(margin))
    pair = jnp.maximum(margin, 0.0) + jnp.log1p(small)
    sigmoid = jnp.where(margin >= 0.0, 1.0, small) / (1.0 + small)
    return -sign * sigmoid * (logit_scale / QUESTION_WORDS), pair


def inner_kernel(
    pbs_ref, pb_ref, live_ref, sign_ref, lse_ref, q_ref, p_ref, page_ref, row_ref, loss_ref, acc_ref,
    qt_ref, weight_ref,
):
    slots, rows = lse_ref.shape
    qt_ref[...] = q_ref[...].T
    pages = pb_ref[:, 0:1]
    first = pages[0:1]
    last = jnp.max(pages, axis=0, keepdims=True)
    values = lse_ref[...]
    for slot in range(slots):
        page_ref[slot : slot + 1, :] = lse_rows(values, pages == pages[slot : slot + 1])
    value = jnp.where(pages >= 0, page_ref[...], 0.0)
    row, pair = gradients(value, sign_ref[...])
    inside = (pages != first) & (pages != last)
    counted = inside & (pages >= 0) & (pb_ref[:, 1:2] == 0)
    row_ref[...] = row
    weight_ref[...] = jnp.where(inside, row, 1.0)
    page_ref[...] = value
    loss = jnp.sum(jnp.where(counted, pair, 0.0), axis=0, keepdims=True)
    loss_ref[...] = jnp.broadcast_to(jnp.sum(loss, axis=1, keepdims=True), loss_ref.shape)
    acc_ref[...] = jnp.zeros_like(acc_ref)
    head_page = pbs_ref[0, 0]
    tail_page = head_page
    for slot in range(1, slots):
        tail_page = jnp.maximum(tail_page, pbs_ref[slot, 0])

    def one(step, carry):
        for half in range(2):
            slot = step * 2 + half
            page = pbs_ref[slot, 0]
            kind = jnp.where(page == head_page, HEAD, jnp.where(page == tail_page, TAIL, INSIDE))
            block = block_of(p_ref, slot)
            for lo in range(0, rows, CHUNK):
                z = scored(qt_ref, block, live_ref, slot, lo)
                weights = jnp.exp2(z - page_ref[pl.ds(slot, 1), lo : lo + CHUNK])
                part = (weight_ref[pl.ds(slot, 1), lo : lo + CHUNK] * weights).astype(bf16)
                acc_ref[kind, :, lo : lo + CHUNK] += lax.dot_general(
                    block, part, (((0,), (0,)), ((), ())), preferred_element_type=f32
                )
        return carry

    lax.fori_loop(0, slots // 2, one, 0)


def close_kernel(
    pb_ref, sign_ref, page_ref, row_ref, loss_ref, acc_ref, recv_ref, out_ref, lse_ref, full_ref
):
    slots, rows = page_ref.shape
    peers = recv_ref.shape[0]
    devices = out_ref.shape[0]
    local = rows // devices
    mine = lax.axis_index("page")
    pages = pb_ref[:, 0:1]
    first = pages[0:1]
    last = jnp.max(pages, axis=0, keepdims=True)
    is_first = pages == first
    is_last = pages == last
    alone = first == last

    def gathered(wanted, below):
        parts = []
        for peer in range(peers):
            side = peer < mine if below else peer > mine
            same = (recv_ref[peer, :, rows : rows + 1] == wanted.astype(f32)) & side
            parts.append(jnp.where(same, recv_ref[peer, :, :rows], very_low))
        peak = parts[0]
        for part in parts[1:]:
            peak = jnp.maximum(peak, part)
        mass = jnp.zeros((1, rows), f32)
        for part in parts:
            mass = mass + jnp.where(part > 0.5 * very_low, jnp.exp2(part - peak), 0.0)
        return peak + jnp.log2(jnp.maximum(mass, 1e-30))

    below = gathered(first, True)
    above = gathered(last, False)
    value = page_ref[...]
    head = value[0:1]
    tail = chosen_row(value, is_last)
    head_full = add_lse(head, below)
    head_full = jnp.where(alone, add_lse(head_full, above), head_full)
    tail_full = jnp.where(alone, head_full, add_lse(tail, above))
    both = jnp.concatenate([head_full, tail_full], axis=0)
    sign = sign_ref[...]
    signs = jnp.concatenate([sign[0:1], chosen_row(sign, is_last)], axis=0)
    row, pair = gradients(both, signs)
    starts = pb_ref[:, 1:2] == 0
    head_counts = starts[0:1]
    tail_counts = (jnp.max((starts & is_last).astype(jnp.int32), axis=0, keepdims=True) > 0) & jnp.logical_not(alone)
    loss = jnp.sum(
        jnp.where(head_counts, pair[0:1], 0.0) + jnp.where(tail_counts, pair[1:2], 0.0),
        axis=1,
        keepdims=True,
    )
    loss = (loss + loss_ref[...]) * (1.0 / QUESTION_WORDS)
    lse_ref[...] = jnp.where(is_last, tail_full, jnp.where(is_first, head_full, value))
    full_ref[...] = jnp.where(is_last, row[1:2], jnp.where(is_first, row[0:1], row_ref[...]))
    head_scale = row[0:1] * jnp.exp2(head - head_full)
    tail_scale = row[1:2] * jnp.exp2(tail - tail_full)
    for lo in range(0, rows, CHUNK):
        span = slice(lo, lo + CHUNK)
        total = (
            acc_ref[INSIDE, :, span]
            + acc_ref[HEAD, :, span] * head_scale[:, span]
            + acc_ref[TAIL, :, span] * tail_scale[:, span]
        )
        turned = total.T.astype(bf16).reshape(CHUNK // local, local, BROWS)
        out_ref[lo // local : (lo + CHUNK) // local, :local, :] = turned
    terms = three_terms(loss)
    zeros = jnp.zeros((LOSS_ROWS - 3, BROWS), f32)
    last_rows = jnp.concatenate([t.astype(f32) for t in terms] + [zeros], axis=0).astype(bf16)
    for device in range(devices):
        out_ref[device, local:, :] = last_rows


def patch_kernel(live_ref, lse_ref, row_ref, q_ref, p_ref, out_ref, qt_ref):
    slots, rows = lse_ref.shape
    qt_ref[...] = q_ref[...].T

    def one(step, carry):
        for half in range(2):
            slot = step * 2 + half
            block = block_of(p_ref, slot)
            total = jnp.zeros((BROWS, BROWS), f32)
            for lo in range(0, rows, CHUNK):
                z = scored(qt_ref, block, live_ref, slot, lo)
                weights = jnp.exp2(z - lse_ref[pl.ds(slot, 1), lo : lo + CHUNK])
                coupling = (row_ref[pl.ds(slot, 1), lo : lo + CHUNK] * weights).astype(bf16)
                total = total + jnp.dot(
                    coupling, q_ref[lo : lo + CHUNK, :], preferred_element_type=f32
                )
            out_ref[pl.ds(pl.multiple_of(slot * BROWS, BROWS), BROWS), :] = total
        return carry

    lax.fori_loop(0, slots // 2, one, 0)


def final_kernel(scale, recv_ref, grad_ref, loss_ref):
    devices, padded, _ = recv_ref.shape
    total = jnp.zeros((padded, BROWS), f32)
    for device in range(devices):
        total = total + recv_ref[device].astype(f32)
    local = padded - LOSS_ROWS
    grad_ref[...] = total[:local]
    loss_ref[...] = (total[local : local + 1] + total[local + 1 : local + 2] + total[local + 2 : local + 3]) * scale


def call(kernel, name, flops, in_specs, shapes, scratch=(), limit=24):
    return pl.pallas_call(
        kernel,
        in_specs=in_specs,
        out_specs=[VMEM] * len(shapes),
        out_shape=[jax.ShapeDtypeStruct(*shape) for shape in shapes],
        scratch_shapes=[pltpu.VMEM(*shape) for shape in scratch],
        cost_estimate=pl.CostEstimate(flops=flops, bytes_accessed=0, transcendentals=0),
        compiler_params=pltpu.CompilerParams(vmem_limit_bytes=limit << 20),
        name=name,
    )


def shards(queries, patches, page_blocks, lengths, labels):
    axes = ("grp", "page")
    devices = lax.axis_size(axes)
    peers = lax.axis_size("page")
    slots = page_blocks.shape[0]
    width = patches.shape[1]
    local_rows = queries.reshape(-1, width)
    local = local_rows.shape[0]
    rows = local * devices
    matmul = 2 * rows * patches.shape[0] * width
    table = ((slots, rows), f32)
    turned = ((width, rows), bf16)
    q = lax.all_to_all(
        jnp.broadcast_to(local_rows[None], (devices, local, width)), axes, 0, 0, tiled=True
    ).reshape(rows, width)
    live, sign = call(
        prep_kernel, "prep", matmul, [VMEM] * 3, [((slots, 128), jnp.int32), table]
    )(page_blocks, lengths.reshape(1, -1), labels)
    lse, send = call(
        stats_kernel, "stats", matmul, [VMEM] * 4, [table, ((peers, 1, rows + 128), f32)], [turned]
    )(page_blocks, live, q, patches)
    recv = lax.all_to_all(send, "page", 0, 0, tiled=True)
    page_lse, row, loss, acc = call(
        inner_kernel,
        "inner",
        2 * matmul,
        [SMEM] + [VMEM] * 6,
        [table, table, ((1, BROWS), f32), ((3, width, rows), f32)],
        [turned, table],
    )(page_blocks, page_blocks, live, sign, lse, q, patches)
    parts, full_lse, row_grad = call(
        close_kernel,
        "close",
        matmul,
        [VMEM] * 7,
        [((devices, local + LOSS_ROWS, width), bf16), table, table],
    )(page_blocks, sign, page_lse, row, loss, acc, recv)
    gathered = lax.all_to_all(parts, axes, 0, 0, tiled=True)
    (patch_grad,) = call(
        patch_kernel, "patch", 2 * matmul, [VMEM] * 5, [(patches.shape, f32)], [turned]
    )(live, full_lse, row_grad, q, patches)
    query_grad, loss = call(
        lambda *refs: final_kernel(QUESTION_WORDS / rows, *refs),
        "final",
        devices * local * width,
        [VMEM],
        [((local, width), f32), ((1, BROWS), f32)],
    )(gathered)
    return (patch_grad, query_grad.reshape(queries.shape), loss[0, :1])


def solution(mesh):
    placed = (
        P(("grp", "page"), None, None),
        P(("grp", "page"), None),
        P(("grp", "page"), None),
        P(),
        P(),
    )
    return jax.shard_map(
        shards,
        mesh=mesh,
        in_specs=placed,
        out_specs=(P(("grp", "page"), None), P(("grp", "page"), None, None), P()),
        check_vma=False,
    )
```

```python
import functools

import jax
import jax.numpy as jnp
from jax import lax
from jax.experimental import pallas as pl
from jax.experimental.pallas import tpu as pltpu
from jax.sharding import PartitionSpec as P

QUESTION_WORDS = 32
BROWS = 128

smoothing_divisor = 0.05
logit_scale = 10.0
logit_bias = -4.0
very_low = -1e30
LOG2E = 1.4426950408889634
LN2 = 0.6931471805599453
SCALE2 = LOG2E / smoothing_divisor
CHUNK = 256
LOSS_ROWS = 8
GROUP = 4
INNER_UNROLL = 1
DEAD = -(2.0**93)
INSIDE, HEAD, TAIL = 0, 1, 2

f32 = jnp.float32
bf16 = jnp.bfloat16
VMEM = pl.BlockSpec(memory_space=pltpu.VMEM)
SMEM = pl.BlockSpec(memory_space=pltpu.SMEM)
HBM = pl.BlockSpec(memory_space=pltpu.HBM)


def lse_rows(values, mask):
    peak = jnp.max(jnp.where(mask, values, very_low), axis=0, keepdims=True)
    mass = jnp.sum(jnp.where(mask, jnp.exp2(values - peak), 0.0), axis=0, keepdims=True)
    return peak + jnp.log2(mass)


def add_lse(one, two):
    peak = jnp.maximum(one, two)
    return peak + jnp.log2(jnp.exp2(one - peak) + jnp.exp2(two - peak))


def chosen_row(values, mask):
    return jnp.max(jnp.where(mask, values, very_low), axis=0, keepdims=True)


def three_terms(value):
    high = value.astype(bf16)
    rest = value - high.astype(f32)
    mid = rest.astype(bf16)
    return high, mid, (rest - mid.astype(f32)).astype(bf16)


def block_of(p_ref, slot):
    return p_ref[pl.ds(pl.multiple_of(slot * BROWS, BROWS), BROWS), :]


def masked(z, live_ref, slot):
    rows = lax.broadcasted_iota(jnp.int32, z.shape, 0)
    live = jnp.concatenate([live_ref[pl.ds(slot, 1), :]] * (z.shape[1] // BROWS), axis=1)
    return jnp.where(rows < live, z, DEAD)


def columns(row, count):
    diagonal = lax.broadcasted_iota(jnp.int32, (count, count), 0) == lax.broadcasted_iota(
        jnp.int32, (count, count), 1
    )
    spread = jnp.where(diagonal, jnp.broadcast_to(row, (count, count)), 0).astype(f32)
    return jnp.sum(spread, axis=1, keepdims=True).astype(jnp.int32)


def slot_stats(live_ref, q_ref, p_ref, lse_ref, qt_ref, base):
    slots = lse_ref.shape[0]
    qt_ref[...] = q_ref[...].T

    def one(step, carry):
        start = step * GROUP
        blocks = p_ref[pl.ds(pl.multiple_of(start * BROWS, BROWS), GROUP * BROWS), :]
        for lo in range(0, q_ref.shape[0], CHUNK):
            product = jnp.dot(blocks, qt_ref[:, lo : lo + CHUNK], preferred_element_type=f32)
            for part in range(GROUP):
                slot = start + part
                z = masked(product[part * BROWS : (part + 1) * BROWS], live_ref, slot)
                top = jnp.max(z, axis=0, keepdims=True)
                mass = jnp.sum(jnp.exp2((z - top) * SCALE2), axis=0, keepdims=True)
                lse_ref[pl.ds(slot, 1), base + lo : base + lo + CHUNK] = top * SCALE2 + jnp.log2(mass)
        return carry

    steps = slots // GROUP
    lax.fori_loop(0, steps, one, 0, unroll=steps if q_ref.shape[0] <= 1024 else 1)


def start_kernel(
    pbt_hbm, len_hbm, p_hbm, rows_hbm, spread_ref, live_ref, page_ref, number_ref, p_ref, pbt_ref, len_ref, rows_ref,
    sems,
):
    slots = live_ref.shape[0]
    pairs = ((rows_hbm, rows_ref), (pbt_hbm, pbt_ref), (len_hbm, len_ref), (p_hbm, p_ref))
    copies = [pltpu.make_async_copy(*pair, sems.at[at]) for at, pair in enumerate(pairs)]
    for copy in copies:
        copy.start()
    for copy in copies[:-1]:
        copy.wait()
    spread_ref[...] = jnp.broadcast_to(rows_ref[...][None], spread_ref.shape)
    pages = columns(pbt_ref[0:1, :], slots)
    numbers = columns(pbt_ref[1:2, :], slots)
    page_count = len_ref.shape[1]
    hit = lax.broadcasted_iota(jnp.int32, (slots, page_count), 1) == pages
    length = jnp.sum(jnp.where(hit, len_ref[...], 0).astype(f32), axis=1, keepdims=True)
    live = length.astype(jnp.int32) - numbers * BROWS
    live_ref[...] = jnp.broadcast_to(jnp.where(pages < 0, 0, live), live_ref.shape)
    page_ref[...] = jnp.broadcast_to(pages, page_ref.shape)
    number_ref[...] = jnp.broadcast_to(numbers, number_ref.shape)
    copies[-1].wait()


def own_kernel(live_ref, q_ref, p_ref, lse_ref, qt_ref):
    slot_stats(live_ref, q_ref, p_ref, lse_ref, qt_ref, 0)


def stats_kernel(
    ids_ref, live_ref, own_lse_ref, q_ref, p_ref, lse_ref, send_ref, qt_ref
):
    slots, rows = lse_ref.shape
    half = rows // 2
    lse_ref[:, :half] = own_lse_ref[...]
    slot_stats(live_ref, q_ref, p_ref, lse_ref, qt_ref, half)
    pages = ids_ref[:, 0:1]
    first = pages[0:1]
    last = jnp.max(pages, axis=0, keepdims=True)
    values = lse_ref[...]
    head = lse_rows(values, pages == first)
    tail = lse_rows(values, pages == last)
    mine = lax.axis_index("page")
    for peer in range(send_ref.shape[0]):
        up = peer > mine
        send_ref[peer, :, :rows] = jnp.where(up, tail, head)
        send_ref[peer, :, rows:] = jnp.broadcast_to(jnp.where(up, last, first).astype(f32), (1, 128))


def label_signs(pages, lab_ref, rows, local):
    slots = pages.shape[0]
    queries, page_count = lab_ref.shape
    half = rows // 2
    core = lax.axis_index("page") % 2
    hit = lax.broadcasted_iota(jnp.int32, (slots, page_count), 1) == pages
    picked = lax.dot_general(
        hit.astype(bf16),
        lab_ref[...].astype(bf16),
        (((1,), (1,)), ((), ())),
        preferred_element_type=f32,
    )
    lane = lax.broadcasted_iota(jnp.int32, (queries, rows), 1)
    other = (lane >= half).astype(jnp.int32)
    within = lane - other * half
    device = 2 * (within // local) + (core + other) % 2
    question = device * (local // QUESTION_WORDS) + within % local // QUESTION_WORDS
    spread = (question == lax.broadcasted_iota(jnp.int32, (queries, rows), 0)).astype(bf16)
    return 2.0 * jnp.dot(picked.astype(bf16), spread, preferred_element_type=f32) - 1.0


def gradients(value, sign):
    count, rows = value.shape
    same_group = (
        lax.broadcasted_iota(jnp.int32, (CHUNK, CHUNK), 0) // QUESTION_WORDS
        == lax.broadcasted_iota(jnp.int32, (CHUNK, CHUNK), 1) // QUESTION_WORDS
    ).astype(bf16)
    totals = []
    for lo in range(0, rows, CHUNK):
        total = [
            jnp.dot(term, same_group, preferred_element_type=f32)
            for term in three_terms(value[:, lo : lo + CHUNK])
        ]
        totals.append(total[0] + total[1] + total[2])
    scores = (smoothing_divisor * LN2) * jnp.concatenate(totals, axis=1)
    logits = (logit_scale / QUESTION_WORDS) * scores + logit_bias
    margin = -sign * logits
    small = jnp.exp(-jnp.abs(margin))
    pair = jnp.maximum(margin, 0.0) + jnp.log1p(small)
    sigmoid = jnp.where(margin >= 0.0, 1.0, small) / (1.0 + small)
    return -sign * sigmoid * (logit_scale / QUESTION_WORDS), pair


def inner_kernel(
    local, pbs_ref, ids_ref, number_ref, live_ref, lab_ref, lse_ref, own_ref, oth_ref, p_ref, page_ref,
    row_ref, sign_ref, loss_ref, acc_ref, weight_ref, qt_ref,
):
    slots, rows = lse_ref.shape
    half = rows // 2
    pages = ids_ref[:, 0:1]
    first = pages[0:1]
    last = jnp.max(pages, axis=0, keepdims=True)
    values = lse_ref[...]
    qt_ref[:, :half] = own_ref[...].T
    qt_ref[:, half:] = oth_ref[...].T
    sign_ref[...] = label_signs(pages, lab_ref, rows, local)
    for slot in range(slots):
        page_ref[slot : slot + 1, :] = chosen_row(values, pages == pages[slot : slot + 1])
    peak = page_ref[...]
    square = jnp.broadcast_to(pages, (slots, slots))
    diagonal = lax.broadcasted_iota(jnp.int32, (slots, slots), 0) == lax.broadcasted_iota(
        jnp.int32, (slots, slots), 1
    )
    across = jnp.sum(jnp.where(diagonal, square, 0).astype(f32), axis=0, keepdims=True)
    same_page = (square.astype(f32) == across).astype(bf16)
    mass = [
        jnp.dot(same_page, term, preferred_element_type=f32)
        for term in three_terms(jnp.exp2(values - peak))
    ]
    value = jnp.where(pages >= 0, peak + jnp.log2(mass[0] + mass[1] + mass[2]), 0.0)
    row, pair = gradients(value, sign_ref[...])
    inside = (pages != first) & (pages != last)
    counted = inside & (pages >= 0) & (number_ref[:, 0:1] == 0)
    row_ref[...] = row
    weight_ref[...] = jnp.where(inside, row, 1.0)
    page_ref[...] = value
    loss = jnp.sum(jnp.where(counted, pair, 0.0), axis=0, keepdims=True)
    loss_ref[...] = jnp.broadcast_to(jnp.sum(loss, axis=1, keepdims=True), loss_ref.shape)
    acc_ref[...] = jnp.zeros_like(acc_ref)
    head_page = pbs_ref[0, 0]
    tail_page = head_page
    for slot in range(1, slots):
        tail_page = jnp.maximum(tail_page, pbs_ref[0, slot])

    def one(step, carry):
        start = step * GROUP
        blocks = p_ref[pl.ds(pl.multiple_of(start * BROWS, BROWS), GROUP * BROWS), :]
        kinds, turned = [], []
        for part in range(GROUP):
            page = pbs_ref[0, start + part]
            kinds.append(jnp.where(page == head_page, HEAD, jnp.where(page == tail_page, TAIL, INSIDE)))
            turned.append(blocks[part * BROWS : (part + 1) * BROWS].T)
        for lo in range(0, rows, CHUNK):
            product = jnp.dot(blocks, qt_ref[:, lo : lo + CHUNK], preferred_element_type=f32)
            for part in range(GROUP):
                slot = start + part
                at = pl.ds(slot, 1)
                z = masked(product[part * BROWS : (part + 1) * BROWS], live_ref, slot)
                e = jnp.exp2(z * SCALE2 - page_ref[at, lo : lo + CHUNK])
                coupling = (e * weight_ref[at, lo : lo + CHUNK]).astype(bf16)
                acc_ref[kinds[part], :, lo : lo + CHUNK] += jnp.dot(
                    turned[part], coupling, preferred_element_type=f32
                )
        return carry

    steps = slots // GROUP
    lax.fori_loop(0, steps, one, 0, unroll=INNER_UNROLL if rows <= 1024 else 1)


def close_kernel(
    ids_ref, number_ref, sign_ref, page_ref, row_ref, loss_ref, acc_ref, recv_ref, out_ref, lse_ref, full_ref
):
    slots, rows = page_ref.shape
    peers = recv_ref.shape[0]
    devices = out_ref.shape[0]
    local = rows // devices
    mine = lax.axis_index("page")
    core = mine % 2
    half = rows // 2
    pages = ids_ref[:, 0:1]
    first = pages[0:1]
    last = jnp.max(pages, axis=0, keepdims=True)
    is_first = pages == first
    is_last = pages == last
    alone = first == last

    def gathered(wanted, below):
        parts = []
        for peer in range(peers):
            side = peer < mine if below else peer > mine
            same = (recv_ref[peer, :, rows : rows + 1] == wanted.astype(f32)) & side
            row = recv_ref[peer, :, :rows]
            crossed = jnp.concatenate([row[:, half:], row[:, :half]], axis=1)
            row = jnp.where(peer % 2 == core, row, crossed)
            parts.append(jnp.where(same, row, very_low))
        peak = parts[0]
        for part in parts[1:]:
            peak = jnp.maximum(peak, part)
        mass = jnp.zeros((1, rows), f32)
        for part in parts:
            mass = mass + jnp.where(part > 0.5 * very_low, jnp.exp2(part - peak), 0.0)
        return peak + jnp.log2(jnp.maximum(mass, 1e-30))

    below = gathered(first, True)
    above = gathered(last, False)
    value = page_ref[...]
    head = value[0:1]
    tail = chosen_row(value, is_last)
    head_full = add_lse(head, below)
    head_full = jnp.where(alone, add_lse(head_full, above), head_full)
    tail_full = jnp.where(alone, head_full, add_lse(tail, above))
    both = jnp.concatenate([head_full, tail_full], axis=0)
    sign = sign_ref[...]
    signs = jnp.concatenate([sign[0:1], chosen_row(sign, is_last)], axis=0)
    row, pair = gradients(both, signs)
    starts = number_ref[:, 0:1] == 0
    head_counts = starts[0:1]
    tail_counts = (jnp.max((starts & is_last).astype(jnp.int32), axis=0, keepdims=True) > 0) & jnp.logical_not(alone)
    loss = jnp.sum(
        jnp.where(head_counts, pair[0:1], 0.0) + jnp.where(tail_counts, pair[1:2], 0.0),
        axis=1,
        keepdims=True,
    )
    loss = (loss + loss_ref[...]) * (1.0 / QUESTION_WORDS)
    lse_ref[...] = jnp.where(is_last, tail_full, jnp.where(is_first, head_full, value))
    full_ref[...] = jnp.where(is_last, row[1:2], jnp.where(is_first, row[0:1], row_ref[...]))
    head_scale = row[0:1] * jnp.exp2(head - head_full)
    tail_scale = row[1:2] * jnp.exp2(tail - tail_full)
    for lo in range(0, rows, CHUNK):
        span = slice(lo, lo + CHUNK)
        total = (
            acc_ref[INSIDE, :, span]
            + acc_ref[HEAD, :, span] * head_scale[:, span]
            + acc_ref[TAIL, :, span] * tail_scale[:, span]
        )
        turned = total.T.astype(bf16).reshape(CHUNK // local, local, BROWS)
        other = int(lo >= half)
        for place in range(CHUNK // local):
            chip = (lo - other * half) // local + place
            out_ref[2 * chip + (core + other) % 2, :local, :] = turned[place]
    terms = three_terms(loss)
    zeros = jnp.zeros((LOSS_ROWS - 3, BROWS), f32)
    last_rows = jnp.concatenate([t.astype(f32) for t in terms] + [zeros], axis=0).astype(bf16)
    for device in range(devices):
        out_ref[device, local:, :] = last_rows


def patch_kernel(live_ref, lse_ref, row_ref, own_ref, oth_ref, p_ref, out_ref, qt_ref):
    slots, rows = lse_ref.shape
    half = rows // 2
    qt_ref[:, :half] = own_ref[...].T
    qt_ref[:, half:] = oth_ref[...].T

    def one(step, carry):
        for part in range(2):
            slot = step * 2 + part
            block = block_of(p_ref, slot)
            total = jnp.zeros((BROWS, BROWS), f32)
            for lo in range(0, rows, CHUNK):
                product = jnp.dot(block, qt_ref[:, lo : lo + CHUNK], preferred_element_type=f32)
                z = masked(product, live_ref, slot)
                weights = jnp.exp2(z * SCALE2 - lse_ref[pl.ds(slot, 1), lo : lo + CHUNK])
                coupling = (row_ref[pl.ds(slot, 1), lo : lo + CHUNK] * weights).astype(bf16)
                q_ref, at = (own_ref, lo) if lo < half else (oth_ref, lo - half)
                total = total + jnp.dot(
                    coupling, q_ref[at : at + CHUNK, :], preferred_element_type=f32
                )
            out_ref[pl.ds(pl.multiple_of(slot * BROWS, BROWS), BROWS), :] = total
        return carry

    lax.fori_loop(0, slots // 2, one, 0)


def final_kernel(scale, recv_ref, grad_ref, loss_ref):
    devices, padded, _ = recv_ref.shape
    total = jnp.zeros((padded, BROWS), f32)
    for device in range(devices):
        total = total + recv_ref[device].astype(f32)
    local = padded - LOSS_ROWS
    grad_ref[...] = total[:local]
    loss_ref[...] = (total[local : local + 1] + total[local + 1 : local + 2] + total[local + 2 : local + 3]) * scale


def call(kernel, name, flops, in_specs, shapes, scratch=(), limit=24):
    return pl.pallas_call(
        kernel,
        in_specs=in_specs,
        out_specs=[VMEM] * len(shapes),
        out_shape=[jax.ShapeDtypeStruct(*shape) for shape in shapes],
        scratch_shapes=[pltpu.VMEM(*shape) if isinstance(shape, tuple) else shape for shape in scratch],
        cost_estimate=pl.CostEstimate(flops=flops, bytes_accessed=0, transcendentals=0),
        compiler_params=pltpu.CompilerParams(vmem_limit_bytes=limit << 20),
        name=name,
    )


def shards(queries, patches, page_blocks, lengths, labels):
    axes = ("grp", "page")
    devices = lax.axis_size(axes)
    peers = lax.axis_size("page")
    slots = page_blocks.shape[0]
    width = patches.shape[1]
    local_rows = queries.reshape(-1, width)
    local = local_rows.shape[0]
    rows = local * devices
    matmul = 2 * rows * patches.shape[0] * width
    half = rows // 2
    table = ((slots, rows), f32)
    half_table = ((slots, half), f32)
    ids = ((slots, BROWS), jnp.int32)
    turned_half = ((width, half), bf16)
    limit = 24 if rows <= 1024 else 52
    pbt = page_blocks.T
    same_core = [list(range(core, devices, 2)) for core in range(2)]
    inputs = (pbt, lengths.reshape(1, -1), patches, local_rows)
    spread, live, pages, numbers, p = call(
        start_kernel,
        "start",
        matmul // 4,
        [HBM] * 4,
        [((devices // 2, local, width), bf16), ids, ids, ids, (patches.shape, bf16)],
        [
            (pbt.shape, jnp.int32),
            ((1, lengths.shape[0]), jnp.int32),
            (local_rows.shape, bf16),
            pltpu.SemaphoreType.DMA((4,)),
        ],
    )(*(pltpu.with_memory_space_constraint(x, pltpu.HBM) for x in inputs))
    own = lax.all_to_all(
        spread,
        axes,
        0,
        0,
        axis_index_groups=same_core,
        tiled=True,
    ).reshape(half, width)
    other = lax.ppermute(own, axes, [(i, i ^ 1) for i in range(devices)])
    (own_lse,) = call(
        own_kernel, "own", matmul // 2, [VMEM] * 3, [half_table], [turned_half], limit
    )(live, own, p)
    lse, send = call(
        stats_kernel,
        "stats",
        matmul // 2,
        [VMEM] * 5,
        [table, ((peers, 1, rows + 128), f32)],
        [turned_half],
        limit,
    )(pages, live, own_lse, other, p)
    recv = lax.all_to_all(send, "page", 0, 0, tiled=True)
    page_lse, row, sign, loss, acc = call(
        functools.partial(inner_kernel, local),
        "inner",
        2 * matmul,
        [SMEM] + [VMEM] * 8,
        [table, table, table, ((1, BROWS), f32), ((3, width, rows), f32)],
        [table, ((width, rows), bf16)],
        limit,
    )(pbt, pages, numbers, live, labels, lse, own, other, p)
    parts, full_lse, row_grad = call(
        close_kernel,
        "close",
        matmul,
        [VMEM] * 8,
        [((devices, local + LOSS_ROWS, width), bf16), table, table],
    )(pages, numbers, sign, page_lse, row, loss, acc, recv)
    gathered = lax.all_to_all(parts, axes, 0, 0, tiled=True)
    (patch_grad,) = call(
        patch_kernel, "patch", 2 * matmul, [VMEM] * 6, [(patches.shape, f32)], [((width, rows), bf16)]
    )(live, full_lse, row_grad, own, other, p)
    query_grad, loss = call(
        lambda *refs: final_kernel(QUESTION_WORDS / rows, *refs),
        "final",
        devices * local * width,
        [VMEM],
        [((local, width), f32), ((1, BROWS), f32)],
    )(gathered)
    return (patch_grad, query_grad.reshape(queries.shape), loss[0, :1])


def solution(mesh):
    placed = (
        P(("grp", "page"), None, None),
        P(("grp", "page"), None),
        P(("grp", "page"), None),
        P(),
        P(),
    )
    return jax.shard_map(
        shards,
        mesh=mesh,
        in_specs=placed,
        out_specs=(P(("grp", "page"), None), P(("grp", "page"), None, None), P()),
        check_vma=False,
    )
```

```python
import functools

import jax
import jax.numpy as jnp
from jax import lax
from jax.experimental import pallas as pl
from jax.experimental.pallas import tpu as pltpu
from jax.sharding import PartitionSpec as P

QUESTION_WORDS = 32
BROWS = 128

smoothing_divisor = 0.05
logit_scale = 10.0
logit_bias = -4.0
very_low = -1e30
LOG2E = 1.4426950408889634
LN2 = 0.6931471805599453
SCALE2 = LOG2E / smoothing_divisor
CHUNK = 256
LOSS_ROWS = 8
GROUP = 4
INNER_UNROLL = 1
PATCH_UNROLL = 1
DEAD = -(2.0**93)
INSIDE, HEAD, TAIL = 0, 1, 2

f32 = jnp.float32
bf16 = jnp.bfloat16
VMEM = pl.BlockSpec(memory_space=pltpu.VMEM)
SMEM = pl.BlockSpec(memory_space=pltpu.SMEM)
HBM = pl.BlockSpec(memory_space=pltpu.HBM)


def lse_rows(values, mask):
    peak = jnp.max(jnp.where(mask, values, very_low), axis=0, keepdims=True)
    mass = jnp.sum(jnp.where(mask, jnp.exp2(values - peak), 0.0), axis=0, keepdims=True)
    return peak + jnp.log2(mass)


def add_lse(one, two):
    peak = jnp.maximum(one, two)
    return peak + jnp.log2(jnp.exp2(one - peak) + jnp.exp2(two - peak))


def chosen_row(values, mask):
    return jnp.max(jnp.where(mask, values, very_low), axis=0, keepdims=True)


def three_terms(value):
    high = value.astype(bf16)
    rest = value - high.astype(f32)
    mid = rest.astype(bf16)
    return high, mid, (rest - mid.astype(f32)).astype(bf16)


def block_of(p_ref, slot):
    return p_ref[pl.ds(pl.multiple_of(slot * BROWS, BROWS), BROWS), :]


def masked(z, live_ref, slot):
    rows = lax.broadcasted_iota(jnp.int32, z.shape, 0)
    live = jnp.concatenate([live_ref[pl.ds(slot, 1), :]] * (z.shape[1] // BROWS), axis=1)
    return jnp.where(rows < live, z, DEAD)


def widened(blocks, live_ref, start):
    rows = lax.broadcasted_iota(jnp.int32, (BROWS, BROWS), 0)
    dead = [
        jnp.where(rows < live_ref[pl.ds(start + part, 1), :], 0.0, 1.0).astype(bf16)
        for part in range(blocks.shape[0] // BROWS)
    ]
    return jnp.concatenate([blocks, jnp.concatenate(dead, axis=0)], axis=1)


def marked_queries(qt_ref, q_ref):
    width = q_ref.shape[1]
    qt_ref[:width, :] = q_ref[...].T
    rows = lax.broadcasted_iota(jnp.int32, (BROWS, q_ref.shape[0]), 0)
    qt_ref[width:, :] = jnp.where(rows == 0, DEAD, 0.0).astype(bf16)


def columns(row, count):
    diagonal = lax.broadcasted_iota(jnp.int32, (count, count), 0) == lax.broadcasted_iota(
        jnp.int32, (count, count), 1
    )
    spread = jnp.where(diagonal, jnp.broadcast_to(row, (count, count)), 0).astype(f32)
    return jnp.sum(spread, axis=1, keepdims=True).astype(jnp.int32)


def slot_stats(live_ref, q_ref, p_ref, lse_ref, qt_ref, base):
    slots = lse_ref.shape[0]
    marked_queries(qt_ref, q_ref)

    def one(step, carry):
        start = step * GROUP
        blocks = p_ref[pl.ds(pl.multiple_of(start * BROWS, BROWS), GROUP * BROWS), :]
        blocks = widened(blocks, live_ref, start)
        for lo in range(0, q_ref.shape[0], CHUNK):
            product = jnp.dot(blocks, qt_ref[:, lo : lo + CHUNK], preferred_element_type=f32)
            for part in range(GROUP):
                slot = start + part
                z = product[part * BROWS : (part + 1) * BROWS]
                top = jnp.max(z, axis=0, keepdims=True)
                mass = jnp.sum(jnp.exp2((z - top) * SCALE2), axis=0, keepdims=True)
                lse_ref[pl.ds(slot, 1), base + lo : base + lo + CHUNK] = top * SCALE2 + jnp.log2(mass)
        return carry

    steps = slots // GROUP
    lax.fori_loop(0, steps, one, 0, unroll=steps if q_ref.shape[0] <= 1024 else 1)


def start_kernel(
    pbt_hbm, len_hbm, p_hbm, rows_hbm, spread_ref, live_ref, page_ref, number_ref, p_ref, pbt_ref, len_ref, rows_ref,
    sems,
):
    slots = live_ref.shape[0]
    pairs = ((rows_hbm, rows_ref), (pbt_hbm, pbt_ref), (len_hbm, len_ref), (p_hbm, p_ref))
    copies = [pltpu.make_async_copy(*pair, sems.at[at]) for at, pair in enumerate(pairs)]
    for copy in copies:
        copy.start()
    for copy in copies[:-1]:
        copy.wait()
    spread_ref[...] = jnp.broadcast_to(rows_ref[...][None], spread_ref.shape)
    pages = columns(pbt_ref[0:1, :], slots)
    numbers = columns(pbt_ref[1:2, :], slots)
    page_count = len_ref.shape[1]
    hit = lax.broadcasted_iota(jnp.int32, (slots, page_count), 1) == pages
    length = jnp.sum(jnp.where(hit, len_ref[...], 0).astype(f32), axis=1, keepdims=True)
    live = length.astype(jnp.int32) - numbers * BROWS
    live_ref[...] = jnp.broadcast_to(jnp.where(pages < 0, 0, live), live_ref.shape)
    page_ref[...] = jnp.broadcast_to(pages, page_ref.shape)
    number_ref[...] = jnp.broadcast_to(numbers, number_ref.shape)
    copies[-1].wait()


def own_kernel(live_ref, q_ref, p_ref, lse_ref, qt_ref):
    slot_stats(live_ref, q_ref, p_ref, lse_ref, qt_ref, 0)


def stats_kernel(
    ids_ref, live_ref, own_lse_ref, q_ref, p_ref, lse_ref, send_ref, qt_ref
):
    slots, rows = lse_ref.shape
    half = rows // 2
    lse_ref[:, :half] = own_lse_ref[...]
    slot_stats(live_ref, q_ref, p_ref, lse_ref, qt_ref, half)
    pages = ids_ref[:, 0:1]
    first = pages[0:1]
    last = jnp.max(pages, axis=0, keepdims=True)
    values = lse_ref[...]
    head = lse_rows(values, pages == first)
    tail = lse_rows(values, pages == last)
    mine = lax.axis_index("page")
    for peer in range(send_ref.shape[0]):
        up = peer > mine
        send_ref[peer, :, :rows] = jnp.where(up, tail, head)
        send_ref[peer, :, rows:] = jnp.broadcast_to(jnp.where(up, last, first).astype(f32), (1, 128))


def label_signs(pages, lab_ref, rows, local):
    slots = pages.shape[0]
    queries, page_count = lab_ref.shape
    half = rows // 2
    core = lax.axis_index("page") % 2
    hit = lax.broadcasted_iota(jnp.int32, (slots, page_count), 1) == pages
    picked = lax.dot_general(
        hit.astype(bf16),
        lab_ref[...].astype(bf16),
        (((1,), (1,)), ((), ())),
        preferred_element_type=f32,
    )
    lane = lax.broadcasted_iota(jnp.int32, (queries, rows), 1)
    other = (lane >= half).astype(jnp.int32)
    within = lane - other * half
    device = 2 * (within // local) + (core + other) % 2
    question = device * (local // QUESTION_WORDS) + within % local // QUESTION_WORDS
    spread = (question == lax.broadcasted_iota(jnp.int32, (queries, rows), 0)).astype(bf16)
    return 2.0 * jnp.dot(picked.astype(bf16), spread, preferred_element_type=f32) - 1.0


def gradients(value, sign):
    count, rows = value.shape
    same_group = (
        lax.broadcasted_iota(jnp.int32, (CHUNK, CHUNK), 0) // QUESTION_WORDS
        == lax.broadcasted_iota(jnp.int32, (CHUNK, CHUNK), 1) // QUESTION_WORDS
    ).astype(bf16)
    totals = []
    for lo in range(0, rows, CHUNK):
        total = [
            jnp.dot(term, same_group, preferred_element_type=f32)
            for term in three_terms(value[:, lo : lo + CHUNK])
        ]
        totals.append(total[0] + total[1] + total[2])
    scores = (smoothing_divisor * LN2) * jnp.concatenate(totals, axis=1)
    logits = (logit_scale / QUESTION_WORDS) * scores + logit_bias
    margin = -sign * logits
    small = jnp.exp(-jnp.abs(margin))
    pair = jnp.maximum(margin, 0.0) + jnp.log1p(small)
    sigmoid = jnp.where(margin >= 0.0, 1.0, small) / (1.0 + small)
    return -sign * sigmoid * (logit_scale / QUESTION_WORDS), pair


def inner_kernel(
    local, pbs_ref, ids_ref, number_ref, live_ref, lab_ref, lse_ref, own_ref, oth_ref, p_ref, page_ref,
    row_ref, sign_ref, loss_ref, acc_ref, weight_ref, qt_ref,
):
    slots, rows = lse_ref.shape
    half = rows // 2
    pages = ids_ref[:, 0:1]
    first = pages[0:1]
    last = jnp.max(pages, axis=0, keepdims=True)
    values = lse_ref[...]
    qt_ref[:, :half] = own_ref[...].T
    qt_ref[:, half:] = oth_ref[...].T
    sign_ref[...] = label_signs(pages, lab_ref, rows, local)
    for slot in range(slots):
        page_ref[slot : slot + 1, :] = chosen_row(values, pages == pages[slot : slot + 1])
    peak = page_ref[...]
    square = jnp.broadcast_to(pages, (slots, slots))
    diagonal = lax.broadcasted_iota(jnp.int32, (slots, slots), 0) == lax.broadcasted_iota(
        jnp.int32, (slots, slots), 1
    )
    across = jnp.sum(jnp.where(diagonal, square, 0).astype(f32), axis=0, keepdims=True)
    same_page = (square.astype(f32) == across).astype(bf16)
    mass = [
        jnp.dot(same_page, term, preferred_element_type=f32)
        for term in three_terms(jnp.exp2(values - peak))
    ]
    value = jnp.where(pages >= 0, peak + jnp.log2(mass[0] + mass[1] + mass[2]), 0.0)
    row, pair = gradients(value, sign_ref[...])
    inside = (pages != first) & (pages != last)
    counted = inside & (pages >= 0) & (number_ref[:, 0:1] == 0)
    row_ref[...] = row
    weight_ref[...] = jnp.where(inside, row, 1.0)
    page_ref[...] = value
    loss = jnp.sum(jnp.where(counted, pair, 0.0), axis=0, keepdims=True)
    loss_ref[...] = jnp.broadcast_to(jnp.sum(loss, axis=1, keepdims=True), loss_ref.shape)
    acc_ref[...] = jnp.zeros_like(acc_ref)
    head_page = pbs_ref[0, 0]
    tail_page = head_page
    for slot in range(1, slots):
        tail_page = jnp.maximum(tail_page, pbs_ref[0, slot])

    def one(step, carry):
        start = step * GROUP
        blocks = p_ref[pl.ds(pl.multiple_of(start * BROWS, BROWS), GROUP * BROWS), :]
        kinds, turned = [], []
        for part in range(GROUP):
            page = pbs_ref[0, start + part]
            kinds.append(jnp.where(page == head_page, HEAD, jnp.where(page == tail_page, TAIL, INSIDE)))
            turned.append(blocks[part * BROWS : (part + 1) * BROWS].T)
        for lo in range(0, rows, CHUNK):
            product = jnp.dot(blocks, qt_ref[:, lo : lo + CHUNK], preferred_element_type=f32)
            for part in range(GROUP):
                slot = start + part
                at = pl.ds(slot, 1)
                z = masked(product[part * BROWS : (part + 1) * BROWS], live_ref, slot)
                e = jnp.exp2(z * SCALE2 - page_ref[at, lo : lo + CHUNK])
                coupling = (e * weight_ref[at, lo : lo + CHUNK]).astype(bf16)
                acc_ref[kinds[part], :, lo : lo + CHUNK] += jnp.dot(
                    turned[part], coupling, preferred_element_type=f32
                )
        return carry

    steps = slots // GROUP
    lax.fori_loop(0, steps, one, 0, unroll=INNER_UNROLL if rows <= 1024 else 1)


def close_kernel(
    ids_ref, number_ref, sign_ref, page_ref, row_ref, loss_ref, acc_ref, recv_ref, keep_ref, give_ref, lse_ref,
    full_ref, part_ref,
):
    slots, rows = page_ref.shape
    peers = recv_ref.shape[0]
    local = rows // keep_ref.shape[0]
    mine = lax.axis_index("page")
    core = mine % 2
    half = rows // 2
    pages = ids_ref[:, 0:1]
    first = pages[0:1]
    last = jnp.max(pages, axis=0, keepdims=True)
    is_first = pages == first
    is_last = pages == last
    alone = first == last

    def gathered(wanted, below):
        parts = []
        for peer in range(peers):
            side = peer < mine if below else peer > mine
            same = (recv_ref[peer, :, rows : rows + 1] == wanted.astype(f32)) & side
            row = recv_ref[peer, :, :rows]
            crossed = jnp.concatenate([row[:, half:], row[:, :half]], axis=1)
            row = jnp.where(peer % 2 == core, row, crossed)
            parts.append(jnp.where(same, row, very_low))
        peak = parts[0]
        for part in parts[1:]:
            peak = jnp.maximum(peak, part)
        mass = jnp.zeros((1, rows), f32)
        for part in parts:
            mass = mass + jnp.where(part > 0.5 * very_low, jnp.exp2(part - peak), 0.0)
        return peak + jnp.log2(jnp.maximum(mass, 1e-30))

    below = gathered(first, True)
    above = gathered(last, False)
    value = page_ref[...]
    head = value[0:1]
    tail = chosen_row(value, is_last)
    head_full = add_lse(head, below)
    head_full = jnp.where(alone, add_lse(head_full, above), head_full)
    tail_full = jnp.where(alone, head_full, add_lse(tail, above))
    both = jnp.concatenate([head_full, tail_full], axis=0)
    sign = sign_ref[...]
    signs = jnp.concatenate([sign[0:1], chosen_row(sign, is_last)], axis=0)
    row, pair = gradients(both, signs)
    starts = number_ref[:, 0:1] == 0
    head_counts = starts[0:1]
    tail_counts = (jnp.max((starts & is_last).astype(jnp.int32), axis=0, keepdims=True) > 0) & jnp.logical_not(alone)
    loss = jnp.sum(
        jnp.where(head_counts, pair[0:1], 0.0) + jnp.where(tail_counts, pair[1:2], 0.0),
        axis=1,
        keepdims=True,
    )
    loss = (loss + loss_ref[...]) * (1.0 / QUESTION_WORDS)
    lse_ref[...] = jnp.where(is_last, tail_full, jnp.where(is_first, head_full, value))
    full_ref[...] = jnp.where(is_last, row[1:2], jnp.where(is_first, row[0:1], row_ref[...]))
    head_scale = row[0:1] * jnp.exp2(head - head_full)
    tail_scale = row[1:2] * jnp.exp2(tail - tail_full)
    for lo in range(0, rows, CHUNK):
        span = slice(lo, lo + CHUNK)
        total = (
            acc_ref[INSIDE, :, span]
            + acc_ref[HEAD, :, span] * head_scale[:, span]
            + acc_ref[TAIL, :, span] * tail_scale[:, span]
        )
        turned = total.T.reshape(CHUNK // local, 2, local // 2, BROWS)
        other = int(lo >= half)
        for place in range(CHUNK // local):
            chip = (lo - other * half) // local + place
            target = 2 * chip + (core + other) % 2
            keep_ref[target] = jnp.where(core == 0, turned[place, 0], turned[place, 1])
            give_ref[target] = jnp.where(core == 0, turned[place, 1], turned[place, 0]).astype(bf16)
    part_ref[...] = loss


def join_kernel(keep_ref, give_ref, part_ref, row_ref, out_ref, again_ref):
    devices, count, _ = keep_ref.shape
    again_ref[...] = row_ref[...]
    terms = three_terms(part_ref[...])
    zeros = jnp.zeros((LOSS_ROWS - 3, BROWS), f32)
    last_rows = jnp.concatenate([t.astype(f32) for t in terms] + [zeros], axis=0).astype(bf16)
    for device in range(devices):
        out_ref[device, :count, :] = (keep_ref[device] + give_ref[device].astype(f32)).astype(bf16)
        out_ref[device, count:, :] = last_rows


def patch_kernel(live_ref, lse_ref, row_ref, own_ref, oth_ref, p_ref, out_ref, qt_ref):
    slots, rows = lse_ref.shape
    half = rows // 2
    qt_ref[:, :half] = own_ref[...].T
    qt_ref[:, half:] = oth_ref[...].T

    def one(step, carry):
        start = step * GROUP
        span = pl.ds(pl.multiple_of(start * BROWS, BROWS), GROUP * BROWS)
        blocks = p_ref[span, :]
        total = jnp.zeros((GROUP * BROWS, BROWS), f32)
        for lo in range(0, rows, CHUNK):
            product = jnp.dot(blocks, qt_ref[:, lo : lo + CHUNK], preferred_element_type=f32)
            couplings = []
            for part in range(GROUP):
                at = pl.ds(start + part, 1)
                z = masked(product[part * BROWS : (part + 1) * BROWS], live_ref, start + part)
                weights = jnp.exp2(z * SCALE2 - lse_ref[at, lo : lo + CHUNK])
                couplings.append((row_ref[at, lo : lo + CHUNK] * weights).astype(bf16))
            q_ref, at = (own_ref, lo) if lo < half else (oth_ref, lo - half)
            total = total + jnp.dot(
                jnp.concatenate(couplings, axis=0), q_ref[at : at + CHUNK, :], preferred_element_type=f32
            )
        out_ref[span, :] = total
        return carry

    steps = slots // GROUP
    lax.fori_loop(0, steps, one, 0, unroll=PATCH_UNROLL if rows <= 1024 else 1)


def final_kernel(scale, recv_ref, grad_ref, loss_ref):
    devices, padded, _ = recv_ref.shape
    count = padded - LOSS_ROWS
    totals = [jnp.zeros((padded, BROWS), f32)] * 2
    for device in range(devices):
        totals[device % 2] = totals[device % 2] + recv_ref[device].astype(f32)
    grad_ref[:count, :] = totals[0][:count]
    grad_ref[count:, :] = totals[1][:count]
    both = totals[0][count:] + totals[1][count:]
    loss_ref[...] = (both[0:1] + both[1:2] + both[2:3]) * scale


def call(kernel, name, flops, in_specs, shapes, scratch=(), limit=24):
    return pl.pallas_call(
        kernel,
        in_specs=in_specs,
        out_specs=[VMEM] * len(shapes),
        out_shape=[jax.ShapeDtypeStruct(*shape) for shape in shapes],
        scratch_shapes=[pltpu.VMEM(*shape) if isinstance(shape, tuple) else shape for shape in scratch],
        cost_estimate=pl.CostEstimate(flops=flops, bytes_accessed=0, transcendentals=0),
        compiler_params=pltpu.CompilerParams(vmem_limit_bytes=limit << 20),
        name=name,
    )


def shards(queries, patches, page_blocks, lengths, labels):
    axes = ("grp", "page")
    devices = lax.axis_size(axes)
    peers = lax.axis_size("page")
    slots = page_blocks.shape[0]
    width = patches.shape[1]
    local_rows = queries.reshape(-1, width)
    local = local_rows.shape[0]
    rows = local * devices
    matmul = 2 * rows * patches.shape[0] * width
    half = rows // 2
    table = ((slots, rows), f32)
    half_table = ((slots, half), f32)
    ids = ((slots, BROWS), jnp.int32)
    turned_half = ((width + BROWS, half), bf16)
    limit = 24 if rows <= 1024 else 52
    pbt = page_blocks.T
    same_core = [list(range(core, devices, 2)) for core in range(2)]
    inputs = (pbt, lengths.reshape(1, -1), patches, local_rows)
    spread, live, pages, numbers, p = call(
        start_kernel,
        "start",
        matmul // 4,
        [HBM] * 4,
        [((devices // 2, local, width), bf16), ids, ids, ids, (patches.shape, bf16)],
        [
            (pbt.shape, jnp.int32),
            ((1, lengths.shape[0]), jnp.int32),
            (local_rows.shape, bf16),
            pltpu.SemaphoreType.DMA((4,)),
        ],
    )(*(pltpu.with_memory_space_constraint(x, pltpu.HBM) for x in inputs))
    own = lax.all_to_all(
        spread,
        axes,
        0,
        0,
        axis_index_groups=same_core,
        tiled=True,
    ).reshape(half, width)
    other = lax.ppermute(own, axes, [(i, i ^ 1) for i in range(devices)])
    (own_lse,) = call(
        own_kernel, "own", matmul // 2, [VMEM] * 3, [half_table], [turned_half], limit
    )(live, own, p)
    lse, send = call(
        stats_kernel,
        "stats",
        matmul // 2,
        [VMEM] * 5,
        [table, ((peers, 1, rows + 128), f32)],
        [turned_half],
        limit,
    )(pages, live, own_lse, other, p)
    recv = lax.all_to_all(send, "page", 0, 0, tiled=True)
    page_lse, row, sign, loss, acc = call(
        functools.partial(inner_kernel, local),
        "inner",
        2 * matmul,
        [SMEM] + [VMEM] * 8,
        [table, table, table, ((1, BROWS), f32), ((3, width, rows), f32)],
        [table, ((width, rows), bf16)],
        limit,
    )(pbt, pages, numbers, live, labels, lse, own, other, p)
    keep, give, full_lse, row_grad, part = call(
        close_kernel,
        "close",
        matmul,
        [VMEM] * 8,
        [
            ((devices, local // 2, width), f32),
            ((devices, local // 2, width), bf16),
            table,
            table,
            ((1, BROWS), f32),
        ],
    )(pages, numbers, sign, page_lse, row, loss, acc, recv)
    give = lax.ppermute(give, axes, [(i, i ^ 1) for i in range(devices)])
    parts, row_grad = call(
        join_kernel,
        "join",
        matmul // 8,
        [VMEM] * 4,
        [((devices, local // 2 + LOSS_ROWS, width), bf16), table],
    )(keep, give, part, row_grad)
    gathered = lax.all_to_all(parts, axes, 0, 0, tiled=True)
    (patch_grad,) = call(
        patch_kernel, "patch", 2 * matmul, [VMEM] * 6, [(patches.shape, f32)], [((width, rows), bf16)]
    )(live, full_lse, row_grad, own, other, p)
    query_grad, loss = call(
        lambda *refs: final_kernel(QUESTION_WORDS / rows, *refs),
        "final",
        devices * local * width,
        [VMEM],
        [((local, width), f32), ((1, BROWS), f32)],
    )(gathered)
    return (patch_grad, query_grad.reshape(queries.shape), loss[0, :1])


def solution(mesh):
    placed = (
        P(("grp", "page"), None, None),
        P(("grp", "page"), None),
        P(("grp", "page"), None),
        P(),
        P(),
    )
    return jax.shard_map(
        shards,
        mesh=mesh,
        in_specs=placed,
        out_specs=(P(("grp", "page"), None), P(("grp", "page"), None, None), P()),
        check_vma=False,
    )
```

```python
import jax
import jax.numpy as jnp
from jax import lax
from jax.experimental import pallas as pl
from jax.experimental.pallas import tpu as pltpu
from jax.sharding import PartitionSpec as P

QUESTION_WORDS = 32
HALF_WORDS = QUESTION_WORDS // 2
BROWS = 128

smoothing_divisor = 0.05
logit_scale = 10.0
logit_bias = -4.0
very_low = -1e30
LOG2E = 1.4426950408889634
LN2 = 0.6931471805599453
SCALE2 = LOG2E / smoothing_divisor
CHUNK = 256
LOW_LANES = 64
GROUP = 4
INNER_UNROLL = 1
PATCH_UNROLL = 1
DEAD = -(2.0**93)
INSIDE, HEAD, TAIL = 0, 1, 2

f32 = jnp.float32
bf16 = jnp.bfloat16
VMEM = pl.BlockSpec(memory_space=pltpu.VMEM)
SMEM = pl.BlockSpec(memory_space=pltpu.SMEM)
HBM = pl.BlockSpec(memory_space=pltpu.HBM)


def lse_rows(values, mask):
    peak = jnp.max(jnp.where(mask, values, very_low), axis=0, keepdims=True)
    mass = jnp.sum(jnp.where(mask, jnp.exp2(values - peak), 0.0), axis=0, keepdims=True)
    return peak + jnp.log2(mass)


def add_lse(one, two):
    peak = jnp.maximum(one, two)
    return peak + jnp.log2(jnp.exp2(one - peak) + jnp.exp2(two - peak))


def chosen_row(values, mask):
    return jnp.max(jnp.where(mask, values, very_low), axis=0, keepdims=True)


def three_terms(value):
    high = value.astype(bf16)
    rest = value - high.astype(f32)
    mid = rest.astype(bf16)
    return high, mid, (rest - mid.astype(f32)).astype(bf16)


def block_of(p_ref, slot):
    return p_ref[pl.ds(pl.multiple_of(slot * BROWS, BROWS), BROWS), :]


def masked(z, live_ref, slot):
    rows = lax.broadcasted_iota(jnp.int32, z.shape, 0)
    live = jnp.concatenate([live_ref[pl.ds(slot, 1), :]] * (z.shape[1] // BROWS), axis=1)
    return jnp.where(rows < live, z, DEAD)


def widened(blocks, live_ref, start):
    rows = lax.broadcasted_iota(jnp.int32, (BROWS, BROWS), 0)
    dead = [
        jnp.where(rows < live_ref[pl.ds(start + part, 1), :], 0.0, 1.0).astype(bf16)
        for part in range(blocks.shape[0] // BROWS)
    ]
    return jnp.concatenate([blocks, jnp.concatenate(dead, axis=0)], axis=1)


def marked_queries(qt_ref, q_ref):
    width = q_ref.shape[1]
    qt_ref[:width, :] = q_ref[...].T
    rows = lax.broadcasted_iota(jnp.int32, (BROWS, q_ref.shape[0]), 0)
    qt_ref[width:, :] = jnp.where(rows == 0, DEAD, 0.0).astype(bf16)


def columns(row, count):
    diagonal = lax.broadcasted_iota(jnp.int32, (count, count), 0) == lax.broadcasted_iota(
        jnp.int32, (count, count), 1
    )
    spread = jnp.where(diagonal, jnp.broadcast_to(row, (count, count)), 0).astype(f32)
    return jnp.sum(spread, axis=1, keepdims=True).astype(jnp.int32)


def slot_stats(live_ref, q_ref, p_ref, lse_ref, qt_ref, base):
    slots = lse_ref.shape[0]
    marked_queries(qt_ref, q_ref)

    def one(step, carry):
        start = step * GROUP
        blocks = p_ref[pl.ds(pl.multiple_of(start * BROWS, BROWS), GROUP * BROWS), :]
        blocks = widened(blocks, live_ref, start)
        for lo in range(0, q_ref.shape[0], CHUNK):
            product = jnp.dot(blocks, qt_ref[:, lo : lo + CHUNK], preferred_element_type=f32)
            for part in range(GROUP):
                slot = start + part
                z = product[part * BROWS : (part + 1) * BROWS]
                top = jnp.max(z, axis=0, keepdims=True)
                mass = jnp.sum(jnp.exp2((z - top) * SCALE2), axis=0, keepdims=True)
                lse_ref[pl.ds(slot, 1), base + lo : base + lo + CHUNK] = top * SCALE2 + jnp.log2(mass)
        return carry

    steps = slots // GROUP
    lax.fori_loop(0, steps, one, 0, unroll=steps if q_ref.shape[0] <= 1024 else 1)


def start_kernel(
    rows_hbm, pbt_hbm, len_hbm, p_hbm, spread_ref, live_ref, page_ref, number_ref, p_ref, rows_ref, pbt_ref,
    len_ref, sems,
):
    slots = live_ref.shape[0]
    pairs = ((rows_hbm, rows_ref), (pbt_hbm, pbt_ref), (len_hbm, len_ref), (p_hbm, p_ref))
    copies = [pltpu.make_async_copy(*pair, sems.at[at]) for at, pair in enumerate(pairs)]
    for copy in copies:
        copy.start()
    for copy in copies[:-1]:
        copy.wait()
    spread_ref[...] = jnp.broadcast_to(rows_ref[...][None], spread_ref.shape)
    pages = columns(pbt_ref[0:1, :], slots)
    numbers = columns(pbt_ref[1:2, :], slots)
    page_count = len_ref.shape[1]
    hit = lax.broadcasted_iota(jnp.int32, (slots, page_count), 1) == pages
    length = jnp.sum(jnp.where(hit, len_ref[...], 0).astype(f32), axis=1, keepdims=True)
    live = length.astype(jnp.int32) - numbers * BROWS
    live_ref[...] = jnp.broadcast_to(jnp.where(pages < 0, 0, live), live_ref.shape)
    page_ref[...] = jnp.broadcast_to(pages, page_ref.shape)
    number_ref[...] = jnp.broadcast_to(numbers, number_ref.shape)
    copies[-1].wait()


def own_kernel(live_ref, q_ref, p_ref, lse_ref, qt_ref):
    slot_stats(live_ref, q_ref, p_ref, lse_ref, qt_ref, 0)


def stats_kernel(
    ids_ref, live_ref, own_lse_ref, q_ref, p_ref, lse_ref, send_ref, qt_ref
):
    slots, rows = lse_ref.shape
    half = rows // 2
    lse_ref[:, :half] = own_lse_ref[...]
    slot_stats(live_ref, q_ref, p_ref, lse_ref, qt_ref, half)
    pages = ids_ref[:, 0:1]
    first = pages[0:1]
    last = jnp.max(pages, axis=0, keepdims=True)
    values = lse_ref[...]
    head = lse_rows(values, pages == first)
    tail = lse_rows(values, pages == last)
    mine = lax.axis_index("page")
    for peer in range(send_ref.shape[0]):
        up = peer > mine
        send_ref[peer, :, :rows] = jnp.where(up, tail, head)
        send_ref[peer, :, rows:] = jnp.broadcast_to(jnp.where(up, last, first).astype(f32), (1, 128))


def label_signs(pages, lab_ref, rows):
    slots = pages.shape[0]
    queries, page_count = lab_ref.shape
    half = rows // 2
    hit = lax.broadcasted_iota(jnp.int32, (slots, page_count), 1) == pages
    picked = lax.dot_general(
        hit.astype(bf16),
        lab_ref[...].astype(bf16),
        (((1,), (1,)), ((), ())),
        preferred_element_type=f32,
    )
    lane = lax.broadcasted_iota(jnp.int32, (queries, rows), 1)
    question = (lane - jnp.where(lane >= half, half, 0)) // HALF_WORDS
    spread = (question == lax.broadcasted_iota(jnp.int32, (queries, rows), 0)).astype(bf16)
    return 2.0 * jnp.dot(picked.astype(bf16), spread, preferred_element_type=f32) - 1.0


def gradients(value, sign):
    count, rows = value.shape
    half = rows // 2
    same_group = (
        lax.broadcasted_iota(jnp.int32, (CHUNK, CHUNK), 0) // HALF_WORDS
        == lax.broadcasted_iota(jnp.int32, (CHUNK, CHUNK), 1) // HALF_WORDS
    ).astype(bf16)
    totals = []
    for lo in range(0, half, CHUNK):
        total = [
            jnp.dot(term, same_group, preferred_element_type=f32)
            for at in (lo, half + lo)
            for term in three_terms(value[:, at : at + CHUNK])
        ]
        totals.append(total[0] + total[1] + total[2] + (total[3] + total[4] + total[5]))
    totals = totals + totals
    scores = (smoothing_divisor * LN2) * jnp.concatenate(totals, axis=1)
    logits = (logit_scale / QUESTION_WORDS) * scores + logit_bias
    margin = -sign * logits
    small = jnp.exp(-jnp.abs(margin))
    pair = jnp.maximum(margin, 0.0) + jnp.log1p(small)
    sigmoid = jnp.where(margin >= 0.0, 1.0, small) / (1.0 + small)
    return -sign * sigmoid * (logit_scale / QUESTION_WORDS), pair


def inner_kernel(
    pbs_ref, ids_ref, number_ref, live_ref, lab_ref, lse_ref, own_ref, oth_ref, p_ref, page_ref,
    row_ref, sign_ref, loss_ref, acc_ref, weight_ref, qt_ref,
):
    slots, rows = lse_ref.shape
    half = rows // 2
    pages = ids_ref[:, 0:1]
    first = pages[0:1]
    last = jnp.max(pages, axis=0, keepdims=True)
    values = lse_ref[...]
    qt_ref[:, :half] = own_ref[...].T
    qt_ref[:, half:] = oth_ref[...].T
    sign_ref[...] = label_signs(pages, lab_ref, rows)
    for slot in range(slots):
        page_ref[slot : slot + 1, :] = chosen_row(values, pages == pages[slot : slot + 1])
    peak = page_ref[...]
    square = jnp.broadcast_to(pages, (slots, slots))
    diagonal = lax.broadcasted_iota(jnp.int32, (slots, slots), 0) == lax.broadcasted_iota(
        jnp.int32, (slots, slots), 1
    )
    across = jnp.sum(jnp.where(diagonal, square, 0).astype(f32), axis=0, keepdims=True)
    same_page = (square.astype(f32) == across).astype(bf16)
    mass = [
        jnp.dot(same_page, term, preferred_element_type=f32)
        for term in three_terms(jnp.exp2(values - peak))
    ]
    value = jnp.where(pages >= 0, peak + jnp.log2(mass[0] + mass[1] + mass[2]), 0.0)
    row, pair = gradients(value, sign_ref[...])
    inside = (pages != first) & (pages != last)
    counted = inside & (pages >= 0) & (number_ref[:, 0:1] == 0)
    row_ref[...] = row
    weight_ref[...] = jnp.where(inside, row, 1.0)
    page_ref[...] = value
    loss = jnp.sum(jnp.where(counted, pair, 0.0), axis=0, keepdims=True)
    loss_ref[...] = jnp.broadcast_to(jnp.sum(loss, axis=1, keepdims=True), loss_ref.shape)
    acc_ref[...] = jnp.zeros_like(acc_ref)
    head_page = pbs_ref[0, 0]
    tail_page = head_page
    for slot in range(1, slots):
        tail_page = jnp.maximum(tail_page, pbs_ref[0, slot])

    def one(step, carry):
        start = step * GROUP
        blocks = p_ref[pl.ds(pl.multiple_of(start * BROWS, BROWS), GROUP * BROWS), :]
        kinds, turned = [], []
        for part in range(GROUP):
            page = pbs_ref[0, start + part]
            kinds.append(jnp.where(page == head_page, HEAD, jnp.where(page == tail_page, TAIL, INSIDE)))
            turned.append(blocks[part * BROWS : (part + 1) * BROWS].T)
        for lo in range(0, rows, CHUNK):
            product = jnp.dot(blocks, qt_ref[:, lo : lo + CHUNK], preferred_element_type=f32)
            for part in range(GROUP):
                slot = start + part
                at = pl.ds(slot, 1)
                z = masked(product[part * BROWS : (part + 1) * BROWS], live_ref, slot)
                e = jnp.exp2(z * SCALE2 - page_ref[at, lo : lo + CHUNK])
                coupling = (e * weight_ref[at, lo : lo + CHUNK]).astype(bf16)
                acc_ref[kinds[part], :, lo : lo + CHUNK] += jnp.dot(
                    turned[part], coupling, preferred_element_type=f32
                )
        return carry

    steps = slots // GROUP
    lax.fori_loop(0, steps, one, 0, unroll=INNER_UNROLL if rows <= 1024 else 1)


def close_kernel(
    ids_ref, number_ref, sign_ref, page_ref, row_ref, loss_ref, acc_ref, recv_ref, keep_ref, give_ref, lse_ref,
    full_ref, part_ref,
):
    slots, rows = page_ref.shape
    peers = recv_ref.shape[0]
    mine = lax.axis_index("page")
    core = mine % 2
    half = rows // 2
    pages = ids_ref[:, 0:1]
    first = pages[0:1]
    last = jnp.max(pages, axis=0, keepdims=True)
    is_first = pages == first
    is_last = pages == last
    alone = first == last

    def gathered(wanted, below):
        parts = []
        for peer in range(peers):
            side = peer < mine if below else peer > mine
            same = (recv_ref[peer, :, rows : rows + 1] == wanted.astype(f32)) & side
            row = recv_ref[peer, :, :rows]
            crossed = jnp.concatenate([row[:, half:], row[:, :half]], axis=1)
            row = jnp.where(peer % 2 == core, row, crossed)
            parts.append(jnp.where(same, row, very_low))
        peak = parts[0]
        for part in parts[1:]:
            peak = jnp.maximum(peak, part)
        mass = jnp.zeros((1, rows), f32)
        for part in parts:
            mass = mass + jnp.where(part > 0.5 * very_low, jnp.exp2(part - peak), 0.0)
        return peak + jnp.log2(jnp.maximum(mass, 1e-30))

    below = gathered(first, True)
    above = gathered(last, False)
    value = page_ref[...]
    head = value[0:1]
    tail = chosen_row(value, is_last)
    head_full = add_lse(head, below)
    head_full = jnp.where(alone, add_lse(head_full, above), head_full)
    tail_full = jnp.where(alone, head_full, add_lse(tail, above))
    both = jnp.concatenate([head_full, tail_full], axis=0)
    sign = sign_ref[...]
    signs = jnp.concatenate([sign[0:1], chosen_row(sign, is_last)], axis=0)
    row, pair = gradients(both, signs)
    starts = number_ref[:, 0:1] == 0
    head_counts = starts[0:1]
    tail_counts = (jnp.max((starts & is_last).astype(jnp.int32), axis=0, keepdims=True) > 0) & jnp.logical_not(alone)
    loss = jnp.sum(
        jnp.where(head_counts, pair[0:1], 0.0) + jnp.where(tail_counts, pair[1:2], 0.0),
        axis=1,
        keepdims=True,
    )
    loss = (loss + loss_ref[...]) * (1.0 / QUESTION_WORDS)
    lse_ref[...] = jnp.where(is_last, tail_full, jnp.where(is_first, head_full, value))
    full_ref[...] = jnp.where(is_last, row[1:2], jnp.where(is_first, row[0:1], row_ref[...]))
    head_scale = row[0:1] * jnp.exp2(head - head_full)
    tail_scale = row[1:2] * jnp.exp2(tail - tail_full)
    for lo in range(0, rows, CHUNK):
        span = slice(lo, lo + CHUNK)
        total = (
            acc_ref[INSIDE, :, span]
            + acc_ref[HEAD, :, span] * head_scale[:, span]
            + acc_ref[TAIL, :, span] * tail_scale[:, span]
        )
        side, at = (keep_ref, lo) if lo < half else (give_ref, lo - half)
        side[at : at + CHUNK, :] = total.T
    part_ref[...] = loss


def join_kernel(keep_ref, give_ref, part_ref, row_ref, out_ref, again_ref):
    devices, pairs = out_ref.shape[0], out_ref.shape[1] - 1
    again_ref[...] = row_ref[...]
    high, mid, low = (term.astype(f32) for term in three_terms(part_ref[...]))
    lane = lax.broadcasted_iota(jnp.int32, (1, BROWS), 1)
    loss = jnp.concatenate([jnp.where(lane < LOW_LANES, high, mid), low], axis=0).astype(bf16)
    for device in range(devices):
        base = device * 2 * pairs
        total = keep_ref[base : base + 2 * pairs, :] + give_ref[base : base + 2 * pairs, :]
        for pair in range(pairs):
            out_ref[device, pair] = total[2 * pair : 2 * pair + 2].astype(bf16)
        out_ref[device, pairs] = loss


def patch_kernel(live_ref, lse_ref, row_ref, own_ref, oth_ref, p_ref, out_ref, qt_ref):
    slots, rows = lse_ref.shape
    half = rows // 2
    qt_ref[:, :half] = own_ref[...].T
    qt_ref[:, half:] = oth_ref[...].T

    def one(step, carry):
        start = step * GROUP
        span = pl.ds(pl.multiple_of(start * BROWS, BROWS), GROUP * BROWS)
        blocks = p_ref[span, :]
        total = jnp.zeros((GROUP * BROWS, BROWS), f32)
        for lo in range(0, rows, CHUNK):
            product = jnp.dot(blocks, qt_ref[:, lo : lo + CHUNK], preferred_element_type=f32)
            couplings = []
            for part in range(GROUP):
                at = pl.ds(start + part, 1)
                z = masked(product[part * BROWS : (part + 1) * BROWS], live_ref, start + part)
                weights = jnp.exp2(z * SCALE2 - lse_ref[at, lo : lo + CHUNK])
                couplings.append((row_ref[at, lo : lo + CHUNK] * weights).astype(bf16))
            q_ref, at = (own_ref, lo) if lo < half else (oth_ref, lo - half)
            total = total + jnp.dot(
                jnp.concatenate(couplings, axis=0), q_ref[at : at + CHUNK, :], preferred_element_type=f32
            )
        out_ref[span, :] = total
        return carry

    steps = slots // GROUP
    lax.fori_loop(0, steps, one, 0, unroll=PATCH_UNROLL if rows <= 1024 else 1)


def final_kernel(scale, recv_ref, grad_ref, loss_ref):
    devices, pairs = recv_ref.shape[0], recv_ref.shape[1] - 1
    totals = [jnp.zeros((pairs + 1, 2, BROWS), f32)] * 2
    for device in range(devices):
        totals[device % 2] = totals[device % 2] + recv_ref[device].astype(f32)
    each = HALF_WORDS // 2
    for core in range(2):
        for pair in range(pairs):
            at = pair % each * 2
            grad_ref[pair // each, core, at : at + 2, :] = totals[core][pair]
    both = totals[0][pairs] + totals[1][pairs]
    loss_ref[...] = (both[0:1, :1] + both[0:1, LOW_LANES : LOW_LANES + 1] + both[1:2]) * scale


def call(kernel, name, flops, in_specs, shapes, scratch=(), limit=24):
    return pl.pallas_call(
        kernel,
        in_specs=in_specs,
        out_specs=[VMEM] * len(shapes),
        out_shape=[jax.ShapeDtypeStruct(*shape) for shape in shapes],
        scratch_shapes=[pltpu.VMEM(*shape) if isinstance(shape, tuple) else shape for shape in scratch],
        cost_estimate=pl.CostEstimate(flops=flops, bytes_accessed=0, transcendentals=0),
        compiler_params=pltpu.CompilerParams(vmem_limit_bytes=limit << 20),
        name=name,
    )


def shards(queries, patches, page_blocks, lengths, labels):
    axes = ("grp", "page")
    devices = lax.axis_size(axes)
    peers = lax.axis_size("page")
    slots = page_blocks.shape[0]
    width = patches.shape[1]
    local_rows = queries.reshape(-1, width)
    local = local_rows.shape[0]
    rows = local * devices
    matmul = 2 * rows * patches.shape[0] * width
    half = rows // 2
    table = ((slots, rows), f32)
    half_table = ((slots, half), f32)
    ids = ((slots, BROWS), jnp.int32)
    turned_half = ((width + BROWS, half), bf16)
    limit = 24 if rows <= 1024 else 52
    pbt = page_blocks.T
    questions = local // QUESTION_WORDS
    halves = local_rows.reshape(questions, 2, HALF_WORDS, width).swapaxes(0, 1).reshape(2, local // 2, width)
    inputs = (halves, page_blocks.T, lengths.reshape(1, -1), patches)
    spread, live, pages, numbers, p = call(
        start_kernel,
        "start",
        matmul // 4,
        [HBM] * 4,
        [((devices // 2, *halves.shape), bf16), ids, ids, ids, (patches.shape, bf16)],
        [
            (halves.shape, bf16),
            (pbt.shape, jnp.int32),
            ((1, lengths.shape[0]), jnp.int32),
            pltpu.SemaphoreType.DMA((4,)),
        ],
    )(*(pltpu.with_memory_space_constraint(x, pltpu.HBM) for x in inputs))
    own = lax.all_to_all(
        spread.reshape(devices, local // 2, width), axes, 0, 0, tiled=True
    ).reshape(half, width)
    pairs = [(i, i ^ 1) for i in range(devices)]
    other = lax.ppermute(own, axes, pairs)
    (own_lse,) = call(
        own_kernel, "own", matmul // 2, [VMEM] * 3, [half_table], [turned_half], limit
    )(live, own, p)
    lse, send = call(
        stats_kernel,
        "stats",
        matmul // 2,
        [VMEM] * 5,
        [table, ((peers, 1, rows + 128), f32)],
        [turned_half],
        limit,
    )(pages, live, own_lse, other, p)
    recv = lax.all_to_all(send, "page", 0, 0, tiled=True)
    page_lse, row, sign, loss, acc = call(
        inner_kernel,
        "inner",
        2 * matmul,
        [SMEM] + [VMEM] * 8,
        [table, table, table, ((1, BROWS), f32), ((3, width, rows), f32)],
        [table, ((width, rows), bf16)],
        limit,
    )(pbt, pages, numbers, live, labels, lse, own, other, p)
    keep, give, full_lse, row_grad, part = call(
        close_kernel,
        "close",
        matmul,
        [VMEM] * 8,
        [
            ((half, width), f32),
            ((half, width), f32),
            table,
            table,
            ((1, BROWS), f32),
        ],
    )(pages, numbers, sign, page_lse, row, loss, acc, recv)
    give = lax.ppermute(give, axes, pairs)
    parts, row_grad = call(
        join_kernel,
        "join",
        matmul // 8,
        [VMEM] * 4,
        [((devices, local // 4 + 1, 2, width), bf16), table],
    )(keep, give, part, row_grad)
    gathered = lax.all_to_all(parts, axes, 0, 0, tiled=True)
    (patch_grad,) = call(
        patch_kernel, "patch", 2 * matmul, [VMEM] * 6, [(patches.shape, f32)], [((width, rows), bf16)]
    )(live, full_lse, row_grad, own, other, p)
    query_grad, loss = call(
        lambda *refs: final_kernel(QUESTION_WORDS / rows, *refs),
        "final",
        devices * local * width,
        [VMEM],
        [((questions, 2, HALF_WORDS, width), f32), ((1, BROWS), f32)],
    )(gathered)
    return (patch_grad, query_grad.reshape(queries.shape), loss[0, :1])


def solution(mesh):
    placed = (
        P(("grp", "page"), None, None),
        P(("grp", "page"), None),
        P(("grp", "page"), None),
        P(),
        P(),
    )
    return jax.shard_map(
        shards,
        mesh=mesh,
        in_specs=placed,
        out_specs=(P(("grp", "page"), None), P(("grp", "page"), None, None), P()),
        check_vma=False,
    )
```

```python
import jax
import jax.numpy as jnp
from jax import lax
from jax.experimental import pallas as pl
from jax.experimental.pallas import tpu as pltpu
from jax.sharding import PartitionSpec as P

QUESTION_WORDS = 32
HALF_WORDS = QUESTION_WORDS // 2
BROWS = 128

smoothing_divisor = 0.05
logit_scale = 10.0
logit_bias = -4.0
very_low = -1e30
LOG2E = 1.4426950408889634
LN2 = 0.6931471805599453
SCALE2 = LOG2E / smoothing_divisor
CHUNK = 256
LOW_LANES = 64
GROUP = 4
INNER_UNROLL = 4
PATCH_UNROLL = 1
DEAD = -(2.0**93)
INSIDE, HEAD, TAIL = 0, 1, 2

f32 = jnp.float32
bf16 = jnp.bfloat16
VMEM = pl.BlockSpec(memory_space=pltpu.VMEM)
SMEM = pl.BlockSpec(memory_space=pltpu.SMEM)
HBM = pl.BlockSpec(memory_space=pltpu.HBM)


def lse_rows(values, mask):
    peak = jnp.max(jnp.where(mask, values, very_low), axis=0, keepdims=True)
    mass = jnp.sum(jnp.where(mask, jnp.exp2(values - peak), 0.0), axis=0, keepdims=True)
    return peak + jnp.log2(mass)


def add_lse(one, two):
    peak = jnp.maximum(one, two)
    return peak + jnp.log2(jnp.exp2(one - peak) + jnp.exp2(two - peak))


def chosen_row(values, mask):
    return jnp.max(jnp.where(mask, values, very_low), axis=0, keepdims=True)


def three_terms(value):
    high = value.astype(bf16)
    rest = value - high.astype(f32)
    mid = rest.astype(bf16)
    return high, mid, (rest - mid.astype(f32)).astype(bf16)


def block_of(p_ref, slot):
    return p_ref[pl.ds(pl.multiple_of(slot * BROWS, BROWS), BROWS), :]


def masked(z, live_ref, slot):
    rows = lax.broadcasted_iota(jnp.int32, z.shape, 0)
    live = jnp.concatenate([live_ref[pl.ds(slot, 1), :]] * (z.shape[1] // BROWS), axis=1)
    return jnp.where(rows < live, z, DEAD)


def widened(blocks, live_ref, start):
    rows = lax.broadcasted_iota(jnp.int32, (BROWS, BROWS), 0)
    dead = [
        jnp.where(rows < live_ref[pl.ds(start + part, 1), :], 0.0, 1.0).astype(bf16)
        for part in range(blocks.shape[0] // BROWS)
    ]
    return jnp.concatenate([blocks, jnp.concatenate(dead, axis=0)], axis=1)


def marked_queries(qt_ref, q_ref):
    width = q_ref.shape[1]
    qt_ref[:width, :] = q_ref[...].T
    rows = lax.broadcasted_iota(jnp.int32, (BROWS, q_ref.shape[0]), 0)
    qt_ref[width:, :] = jnp.where(rows == 0, DEAD, 0.0).astype(bf16)


def columns(row, count):
    diagonal = lax.broadcasted_iota(jnp.int32, (count, count), 0) == lax.broadcasted_iota(
        jnp.int32, (count, count), 1
    )
    spread = jnp.where(diagonal, jnp.broadcast_to(row, (count, count)), 0).astype(f32)
    return jnp.sum(spread, axis=1, keepdims=True).astype(jnp.int32)


def slot_stats(live_ref, q_ref, p_ref, lse_ref, qt_ref, base):
    slots = lse_ref.shape[0]
    marked_queries(qt_ref, q_ref)

    def one(step, carry):
        start = step * GROUP
        blocks = p_ref[pl.ds(pl.multiple_of(start * BROWS, BROWS), GROUP * BROWS), :]
        blocks = widened(blocks, live_ref, start)
        for lo in range(0, q_ref.shape[0], CHUNK):
            product = jnp.dot(blocks, qt_ref[:, lo : lo + CHUNK], preferred_element_type=f32)
            for part in range(GROUP):
                slot = start + part
                z = product[part * BROWS : (part + 1) * BROWS]
                top = jnp.max(z, axis=0, keepdims=True)
                mass = jnp.sum(jnp.exp2((z - top) * SCALE2), axis=0, keepdims=True)
                lse_ref[pl.ds(slot, 1), base + lo : base + lo + CHUNK] = top * SCALE2 + jnp.log2(mass)
        return carry

    steps = slots // GROUP
    lax.fori_loop(0, steps, one, 0, unroll=steps if q_ref.shape[0] <= 1024 else 1)


def start_kernel(
    rows_hbm, pbt_hbm, len_hbm, p_hbm, spread_ref, live_ref, page_ref, number_ref, p_ref, rows_ref, pbt_ref,
    len_ref, sems,
):
    slots = live_ref.shape[0]
    pairs = ((rows_hbm, rows_ref), (pbt_hbm, pbt_ref), (len_hbm, len_ref), (p_hbm, p_ref))
    copies = [pltpu.make_async_copy(*pair, sems.at[at]) for at, pair in enumerate(pairs)]
    for copy in copies:
        copy.start()
    for copy in copies[:-1]:
        copy.wait()
    spread_ref[...] = jnp.broadcast_to(rows_ref[...][None], spread_ref.shape)
    pages = columns(pbt_ref[0:1, :], slots)
    numbers = columns(pbt_ref[1:2, :], slots)
    page_count = len_ref.shape[1]
    hit = lax.broadcasted_iota(jnp.int32, (slots, page_count), 1) == pages
    length = jnp.sum(jnp.where(hit, len_ref[...], 0).astype(f32), axis=1, keepdims=True)
    live = length.astype(jnp.int32) - numbers * BROWS
    live_ref[...] = jnp.broadcast_to(jnp.where(pages < 0, 0, live), live_ref.shape)
    page_ref[...] = jnp.broadcast_to(pages, page_ref.shape)
    number_ref[...] = jnp.broadcast_to(numbers, number_ref.shape)
    copies[-1].wait()


def own_kernel(live_ref, q_ref, p_ref, lse_ref, qt_ref):
    slot_stats(live_ref, q_ref, p_ref, lse_ref, qt_ref, 0)


def stats_kernel(
    ids_ref, live_ref, own_lse_ref, q_ref, p_ref, lse_ref, send_ref, qt_ref
):
    slots, rows = lse_ref.shape
    half = rows // 2
    lse_ref[:, :half] = own_lse_ref[...]
    slot_stats(live_ref, q_ref, p_ref, lse_ref, qt_ref, half)
    pages = ids_ref[:, 0:1]
    first = pages[0:1]
    last = jnp.max(pages, axis=0, keepdims=True)
    values = lse_ref[...]
    head = lse_rows(values, pages == first)
    tail = lse_rows(values, pages == last)
    mine = lax.axis_index("page")
    for peer in range(send_ref.shape[0]):
        up = peer > mine
        send_ref[peer, :, :rows] = jnp.where(up, tail, head)
        send_ref[peer, :, rows:] = jnp.broadcast_to(jnp.where(up, last, first).astype(f32), (1, 128))


def label_signs(pages, lab_ref, rows):
    slots = pages.shape[0]
    queries, page_count = lab_ref.shape
    half = rows // 2
    hit = lax.broadcasted_iota(jnp.int32, (slots, page_count), 1) == pages
    picked = lax.dot_general(
        hit.astype(bf16),
        lab_ref[...].astype(bf16),
        (((1,), (1,)), ((), ())),
        preferred_element_type=f32,
    )
    lane = lax.broadcasted_iota(jnp.int32, (queries, rows), 1)
    question = (lane - jnp.where(lane >= half, half, 0)) // HALF_WORDS
    spread = (question == lax.broadcasted_iota(jnp.int32, (queries, rows), 0)).astype(bf16)
    return 2.0 * jnp.dot(picked.astype(bf16), spread, preferred_element_type=f32) - 1.0


def gradients(value, sign):
    count, rows = value.shape
    half = rows // 2
    same_group = (
        lax.broadcasted_iota(jnp.int32, (CHUNK, CHUNK), 0) // HALF_WORDS
        == lax.broadcasted_iota(jnp.int32, (CHUNK, CHUNK), 1) // HALF_WORDS
    ).astype(bf16)
    totals = []
    for lo in range(0, half, CHUNK):
        total = [
            jnp.dot(term, same_group, preferred_element_type=f32)
            for at in (lo, half + lo)
            for term in three_terms(value[:, at : at + CHUNK])
        ]
        totals.append(total[0] + total[1] + total[2] + (total[3] + total[4] + total[5]))
    totals = totals + totals
    scores = (smoothing_divisor * LN2) * jnp.concatenate(totals, axis=1)
    logits = (logit_scale / QUESTION_WORDS) * scores + logit_bias
    margin = -sign * logits
    small = jnp.exp(-jnp.abs(margin))
    pair = jnp.maximum(margin, 0.0) + jnp.log1p(small)
    sigmoid = jnp.where(margin >= 0.0, 1.0, small) / (1.0 + small)
    return -sign * sigmoid * (logit_scale / QUESTION_WORDS), pair


def inner_kernel(
    pbs_ref, ids_ref, number_ref, live_ref, lab_ref, lse_ref, own_ref, oth_ref, p_ref, page_ref,
    row_ref, sign_ref, loss_ref, acc_ref, weight_ref, qt_ref,
):
    slots, rows = lse_ref.shape
    half = rows // 2
    pages = ids_ref[:, 0:1]
    first = pages[0:1]
    last = jnp.max(pages, axis=0, keepdims=True)
    values = lse_ref[...]
    qt_ref[:, :half] = own_ref[...].T
    qt_ref[:, half:] = oth_ref[...].T
    sign_ref[...] = label_signs(pages, lab_ref, rows)
    for slot in range(slots):
        page_ref[slot : slot + 1, :] = chosen_row(values, pages == pages[slot : slot + 1])
    peak = page_ref[...]
    square = jnp.broadcast_to(pages, (slots, slots))
    diagonal = lax.broadcasted_iota(jnp.int32, (slots, slots), 0) == lax.broadcasted_iota(
        jnp.int32, (slots, slots), 1
    )
    across = jnp.sum(jnp.where(diagonal, square, 0).astype(f32), axis=0, keepdims=True)
    same_page = (square.astype(f32) == across).astype(bf16)
    mass = [
        jnp.dot(same_page, term, preferred_element_type=f32)
        for term in three_terms(jnp.exp2(values - peak))
    ]
    value = jnp.where(pages >= 0, peak + jnp.log2(mass[0] + mass[1] + mass[2]), 0.0)
    row, pair = gradients(value, sign_ref[...])
    inside = (pages != first) & (pages != last)
    counted = inside & (pages >= 0) & (number_ref[:, 0:1] == 0)
    row_ref[...] = row
    weight_ref[...] = jnp.where(inside, row, 1.0)
    page_ref[...] = value
    loss = jnp.sum(jnp.where(counted, pair, 0.0), axis=0, keepdims=True)
    loss_ref[...] = jnp.broadcast_to(jnp.sum(loss, axis=1, keepdims=True), loss_ref.shape)
    acc_ref[...] = jnp.zeros_like(acc_ref)
    head_page = pbs_ref[0, 0]
    tail_page = head_page
    for slot in range(1, slots):
        tail_page = jnp.maximum(tail_page, pbs_ref[0, slot])

    def one(step, carry):
        start = step * GROUP
        blocks = p_ref[pl.ds(pl.multiple_of(start * BROWS, BROWS), GROUP * BROWS), :]
        kinds, turned = [], []
        for part in range(GROUP):
            page = pbs_ref[0, start + part]
            kinds.append(jnp.where(page == head_page, HEAD, jnp.where(page == tail_page, TAIL, INSIDE)))
            turned.append(blocks[part * BROWS : (part + 1) * BROWS].T)
        for lo in range(0, rows, CHUNK):
            product = jnp.dot(blocks, qt_ref[:, lo : lo + CHUNK], preferred_element_type=f32)
            for part in range(GROUP):
                slot = start + part
                at = pl.ds(slot, 1)
                z = masked(product[part * BROWS : (part + 1) * BROWS], live_ref, slot)
                e = jnp.exp2(z * SCALE2 - page_ref[at, lo : lo + CHUNK])
                coupling = (e * weight_ref[at, lo : lo + CHUNK]).astype(bf16)
                acc_ref[kinds[part], :, lo : lo + CHUNK] += jnp.dot(
                    turned[part], coupling, preferred_element_type=f32
                )
        return carry

    steps = slots // GROUP
    lax.fori_loop(0, steps, one, 0, unroll=INNER_UNROLL if rows <= 1024 else 1)


def close_kernel(
    ids_ref, number_ref, sign_ref, page_ref, row_ref, loss_ref, acc_ref, recv_ref, scales_ref, give_ref, lse_ref,
    full_ref, part_ref, got_ref,
):
    slots, rows = page_ref.shape
    peers = recv_ref.shape[0]
    mine = lax.axis_index("page")
    core = mine % 2
    half = rows // 2
    pages = ids_ref[:, 0:1]
    first = pages[0:1]
    last = jnp.max(pages, axis=0, keepdims=True)
    is_first = pages == first
    is_last = pages == last
    alone = first == last

    for peer in range(peers):
        got_ref[peer : peer + 1, :] = recv_ref[peer]
    peer = lax.broadcasted_iota(jnp.int32, (peers, 1), 0)
    got = got_ref[:, :rows]
    crossed = jnp.concatenate([got[:, half:], got[:, :half]], axis=1)
    got = jnp.where(peer % 2 == core, got, crossed)
    ids = got_ref[:, rows : rows + 1]

    def gathered(mask):
        peak = chosen_row(got, mask)
        mass = jnp.sum(jnp.where(mask, jnp.exp2(got - peak), 0.0), axis=0, keepdims=True)
        return peak + jnp.log2(jnp.maximum(mass, 1e-30))

    below = gathered((peer < mine) & (ids == first.astype(f32)))
    above = gathered((peer > mine) & (ids == last.astype(f32)))
    value = page_ref[...]
    head = value[0:1]
    tail = chosen_row(value, is_last)
    head_full = add_lse(head, below)
    head_full = jnp.where(alone, add_lse(head_full, above), head_full)
    tail_full = jnp.where(alone, head_full, add_lse(tail, above))
    both = jnp.concatenate([head_full, tail_full], axis=0)
    sign = sign_ref[...]
    signs = jnp.concatenate([sign[0:1], chosen_row(sign, is_last)], axis=0)
    row, pair = gradients(both, signs)
    starts = number_ref[:, 0:1] == 0
    head_counts = starts[0:1]
    tail_counts = (jnp.max((starts & is_last).astype(jnp.int32), axis=0, keepdims=True) > 0) & jnp.logical_not(alone)
    loss = jnp.sum(
        jnp.where(head_counts, pair[0:1], 0.0) + jnp.where(tail_counts, pair[1:2], 0.0),
        axis=1,
        keepdims=True,
    )
    loss = (loss + loss_ref[...]) * (1.0 / QUESTION_WORDS)
    lse_ref[...] = jnp.where(is_last, tail_full, jnp.where(is_first, head_full, value))
    full_ref[...] = jnp.where(is_last, row[1:2], jnp.where(is_first, row[0:1], row_ref[...]))
    head_scale = row[0:1] * jnp.exp2(head - head_full)
    tail_scale = row[1:2] * jnp.exp2(tail - tail_full)
    scales_ref[0:1, :] = head_scale
    scales_ref[1:2, :] = tail_scale
    combine(acc_ref, scales_ref, give_ref, half)
    part_ref[...] = loss


def combine(acc_ref, scales_ref, out_ref, base):
    for lo in range(0, out_ref.shape[0], CHUNK):
        span = slice(base + lo, base + lo + CHUNK)
        total = (
            acc_ref[INSIDE, :, span]
            + acc_ref[HEAD, :, span] * scales_ref[0:1, span]
            + acc_ref[TAIL, :, span] * scales_ref[1:2, span]
        )
        out_ref[lo : lo + CHUNK, :] = total.T


def keep_kernel(acc_ref, scales_ref, keep_ref):
    combine(acc_ref, scales_ref, keep_ref, 0)


def join_kernel(keep_ref, give_ref, part_ref, row_ref, out_ref, again_ref):
    devices, pairs = out_ref.shape[0], out_ref.shape[1] - 1
    again_ref[...] = row_ref[...]
    high, mid, low = (term.astype(f32) for term in three_terms(part_ref[...]))
    lane = lax.broadcasted_iota(jnp.int32, (1, BROWS), 1)
    loss = jnp.concatenate([jnp.where(lane < LOW_LANES, high, mid), low], axis=0).astype(bf16)
    for device in range(devices):
        base = device * 2 * pairs
        total = keep_ref[base : base + 2 * pairs, :] + give_ref[base : base + 2 * pairs, :]
        for pair in range(pairs):
            out_ref[device, pair] = total[2 * pair : 2 * pair + 2].astype(bf16)
        out_ref[device, pairs] = loss


def patch_kernel(live_ref, lse_ref, row_ref, own_ref, oth_ref, p_ref, out_ref, qt_ref):
    slots, rows = lse_ref.shape
    half = rows // 2
    qt_ref[:, :half] = own_ref[...].T
    qt_ref[:, half:] = oth_ref[...].T

    def one(step, carry):
        start = step * GROUP
        span = pl.ds(pl.multiple_of(start * BROWS, BROWS), GROUP * BROWS)
        blocks = p_ref[span, :]
        total = jnp.zeros((GROUP * BROWS, BROWS), f32)
        for lo in range(0, rows, CHUNK):
            product = jnp.dot(blocks, qt_ref[:, lo : lo + CHUNK], preferred_element_type=f32)
            couplings = []
            for part in range(GROUP):
                at = pl.ds(start + part, 1)
                z = masked(product[part * BROWS : (part + 1) * BROWS], live_ref, start + part)
                weights = jnp.exp2(z * SCALE2 - lse_ref[at, lo : lo + CHUNK])
                couplings.append((row_ref[at, lo : lo + CHUNK] * weights).astype(bf16))
            q_ref, at = (own_ref, lo) if lo < half else (oth_ref, lo - half)
            total = total + jnp.dot(
                jnp.concatenate(couplings, axis=0), q_ref[at : at + CHUNK, :], preferred_element_type=f32
            )
        out_ref[span, :] = total
        return carry

    steps = slots // GROUP
    lax.fori_loop(0, steps, one, 0, unroll=PATCH_UNROLL if rows <= 1024 else 1)


def final_kernel(scale, recv_ref, grad_ref, loss_ref):
    devices, pairs = recv_ref.shape[0], recv_ref.shape[1] - 1
    totals = [jnp.zeros((pairs + 1, 2, BROWS), f32)] * 2
    for device in range(devices):
        totals[device % 2] = totals[device % 2] + recv_ref[device].astype(f32)
    each = HALF_WORDS // 2
    for core in range(2):
        for pair in range(pairs):
            at = pair % each * 2
            grad_ref[pair // each, core, at : at + 2, :] = totals[core][pair]
    both = totals[0][pairs] + totals[1][pairs]
    loss_ref[...] = (both[0:1, :1] + both[0:1, LOW_LANES : LOW_LANES + 1] + both[1:2]) * scale


def call(kernel, name, flops, in_specs, shapes, scratch=(), limit=24):
    return pl.pallas_call(
        kernel,
        in_specs=in_specs,
        out_specs=[VMEM] * len(shapes),
        out_shape=[jax.ShapeDtypeStruct(*shape) for shape in shapes],
        scratch_shapes=[pltpu.VMEM(*shape) if isinstance(shape, tuple) else shape for shape in scratch],
        cost_estimate=pl.CostEstimate(flops=flops, bytes_accessed=0, transcendentals=0),
        compiler_params=pltpu.CompilerParams(vmem_limit_bytes=limit << 20),
        name=name,
    )


def shards(queries, patches, page_blocks, lengths, labels):
    axes = ("grp", "page")
    devices = lax.axis_size(axes)
    peers = lax.axis_size("page")
    slots = page_blocks.shape[0]
    width = patches.shape[1]
    local_rows = queries.reshape(-1, width)
    local = local_rows.shape[0]
    rows = local * devices
    matmul = 2 * rows * patches.shape[0] * width
    half = rows // 2
    table = ((slots, rows), f32)
    half_table = ((slots, half), f32)
    ids = ((slots, BROWS), jnp.int32)
    turned_half = ((width + BROWS, half), bf16)
    limit = 24 if rows <= 1024 else 52
    pbt = page_blocks.T
    questions = local // QUESTION_WORDS
    halves = local_rows.reshape(questions, 2, HALF_WORDS, width).swapaxes(0, 1).reshape(2, local // 2, width)
    inputs = (halves, page_blocks.T, lengths.reshape(1, -1), patches)
    spread, live, pages, numbers, p = call(
        start_kernel,
        "start",
        matmul // 4,
        [HBM] * 4,
        [((devices // 2, *halves.shape), bf16), ids, ids, ids, (patches.shape, bf16)],
        [
            (halves.shape, bf16),
            (pbt.shape, jnp.int32),
            ((1, lengths.shape[0]), jnp.int32),
            pltpu.SemaphoreType.DMA((4,)),
        ],
    )(*(pltpu.with_memory_space_constraint(x, pltpu.HBM) for x in inputs))
    own = lax.all_to_all(
        spread.reshape(devices, local // 2, width), axes, 0, 0, tiled=True
    ).reshape(half, width)
    pairs = [(i, i ^ 1) for i in range(devices)]
    other = lax.ppermute(own, axes, pairs)
    (own_lse,) = call(
        own_kernel, "own", matmul // 2, [VMEM] * 3, [half_table], [turned_half], limit
    )(live, own, p)
    lse, send = call(
        stats_kernel,
        "stats",
        matmul // 2,
        [VMEM] * 5,
        [table, ((peers, 1, rows + 128), f32)],
        [turned_half],
        limit,
    )(pages, live, own_lse, other, p)
    recv = lax.all_to_all(send, "page", 0, 0, tiled=True)
    page_lse, row, sign, loss, acc = call(
        inner_kernel,
        "inner",
        2 * matmul,
        [SMEM] + [VMEM] * 8,
        [table, table, table, ((1, BROWS), f32), ((3, width, rows), f32)],
        [table, ((width, rows), bf16)],
        limit,
    )(pbt, pages, numbers, live, labels, lse, own, other, p)
    scales, give, full_lse, row_grad, part = call(
        close_kernel,
        "close",
        matmul,
        [VMEM] * 8,
        [
            ((2, rows), f32),
            ((half, width), f32),
            table,
            table,
            ((1, BROWS), f32),
        ],
        [((peers, rows + 128), f32)],
    )(pages, numbers, sign, page_lse, row, loss, acc, recv)
    give = lax.ppermute(give, axes, pairs)
    (keep,) = call(keep_kernel, "keep", matmul // 4, [VMEM] * 2, [((half, width), f32)])(acc, scales)
    parts, row_grad = call(
        join_kernel,
        "join",
        matmul // 8,
        [VMEM] * 4,
        [((devices, local // 4 + 1, 2, width), bf16), table],
    )(keep, give, part, row_grad)
    gathered = lax.all_to_all(parts, axes, 0, 0, tiled=True)
    (patch_grad,) = call(
        patch_kernel, "patch", 2 * matmul, [VMEM] * 6, [(patches.shape, f32)], [((width, rows), bf16)]
    )(live, full_lse, row_grad, own, other, p)
    query_grad, loss = call(
        lambda *refs: final_kernel(QUESTION_WORDS / rows, *refs),
        "final",
        devices * local * width,
        [VMEM],
        [((questions, 2, HALF_WORDS, width), f32), ((1, BROWS), f32)],
    )(gathered)
    return (patch_grad, query_grad.reshape(queries.shape), loss[0, :1])


def solution(mesh):
    placed = (
        P(("grp", "page"), None, None),
        P(("grp", "page"), None),
        P(("grp", "page"), None),
        P(),
        P(),
    )
    return jax.shard_map(
        shards,
        mesh=mesh,
        in_specs=placed,
        out_specs=(P(("grp", "page"), None), P(("grp", "page"), None, None), P()),
        check_vma=False,
    )
```

```python
import jax
import jax.numpy as jnp
from jax import lax
from jax.experimental import pallas as pl
from jax.experimental.pallas import tpu as pltpu
from jax.sharding import PartitionSpec as P

QUESTION_WORDS = 32
HALF_WORDS = QUESTION_WORDS // 2
BROWS = 128

smoothing_divisor = 0.05
logit_scale = 10.0
logit_bias = -4.0
very_low = -1e30
LOG2E = 1.4426950408889634
LN2 = 0.6931471805599453
SCALE2 = LOG2E / smoothing_divisor
CHUNK = 256
LOW_LANES = 64
GROUP = 4
INNER_UNROLL = 4
PATCH_UNROLL = 1
DEAD = -(2.0**93)
INSIDE, HEAD, TAIL = 0, 1, 2

f32 = jnp.float32
bf16 = jnp.bfloat16
VMEM = pl.BlockSpec(memory_space=pltpu.VMEM)
SMEM = pl.BlockSpec(memory_space=pltpu.SMEM)
HBM = pl.BlockSpec(memory_space=pltpu.HBM)


def lse_rows(values, mask):
    peak = jnp.max(jnp.where(mask, values, very_low), axis=0, keepdims=True)
    mass = jnp.sum(jnp.where(mask, jnp.exp2(values - peak), 0.0), axis=0, keepdims=True)
    return peak + jnp.log2(mass)


def add_lse(one, two):
    peak = jnp.maximum(one, two)
    return peak + jnp.log2(jnp.exp2(one - peak) + jnp.exp2(two - peak))


def chosen_row(values, mask):
    return jnp.max(jnp.where(mask, values, very_low), axis=0, keepdims=True)


def three_terms(value):
    high = value.astype(bf16)
    rest = value - high.astype(f32)
    mid = rest.astype(bf16)
    return high, mid, (rest - mid.astype(f32)).astype(bf16)


def block_of(p_ref, slot):
    return p_ref[pl.ds(pl.multiple_of(slot * BROWS, BROWS), BROWS), :]


def masked(z, live_ref, slot):
    rows = lax.broadcasted_iota(jnp.int32, z.shape, 0)
    live = jnp.concatenate([live_ref[pl.ds(slot, 1), :]] * (z.shape[1] // BROWS), axis=1)
    return jnp.where(rows < live, z, DEAD)


def widened(blocks, live_ref, start):
    rows = lax.broadcasted_iota(jnp.int32, (BROWS, BROWS), 0)
    dead = [
        jnp.where(rows < live_ref[pl.ds(start + part, 1), :], 0.0, 1.0).astype(bf16)
        for part in range(blocks.shape[0] // BROWS)
    ]
    return jnp.concatenate([blocks, jnp.concatenate(dead, axis=0)], axis=1)


def marked_queries(qt_ref, q_ref):
    width = q_ref.shape[1]
    qt_ref[:width, :] = q_ref[...].T
    rows = lax.broadcasted_iota(jnp.int32, (BROWS, q_ref.shape[0]), 0)
    qt_ref[width:, :] = jnp.where(rows == 0, DEAD, 0.0).astype(bf16)


def columns(row, count):
    diagonal = lax.broadcasted_iota(jnp.int32, (count, count), 0) == lax.broadcasted_iota(
        jnp.int32, (count, count), 1
    )
    spread = jnp.where(diagonal, jnp.broadcast_to(row, (count, count)), 0).astype(f32)
    return jnp.sum(spread, axis=1, keepdims=True).astype(jnp.int32)


def slot_stats(live_ref, q_ref, p_ref, lse_ref, qt_ref, base):
    slots = lse_ref.shape[0]
    marked_queries(qt_ref, q_ref)

    def one(step, carry):
        start = step * GROUP
        blocks = p_ref[pl.ds(pl.multiple_of(start * BROWS, BROWS), GROUP * BROWS), :]
        blocks = widened(blocks, live_ref, start)
        for lo in range(0, q_ref.shape[0], CHUNK):
            product = jnp.dot(blocks, qt_ref[:, lo : lo + CHUNK], preferred_element_type=f32)
            for part in range(GROUP):
                slot = start + part
                z = product[part * BROWS : (part + 1) * BROWS]
                top = jnp.max(z, axis=0, keepdims=True)
                mass = jnp.sum(jnp.exp2((z - top) * SCALE2), axis=0, keepdims=True)
                lse_ref[pl.ds(slot, 1), base + lo : base + lo + CHUNK] = top * SCALE2 + jnp.log2(mass)
        return carry

    steps = slots // GROUP
    lax.fori_loop(0, steps, one, 0, unroll=steps if q_ref.shape[0] <= 1024 else 1)


def start_kernel(
    rows_hbm, pbt_hbm, len_hbm, spread_ref, live_ref, page_ref, number_ref, rows_ref, pbt_ref, len_ref, sems,
):
    slots = live_ref.shape[0]
    pairs = ((rows_hbm, rows_ref), (pbt_hbm, pbt_ref), (len_hbm, len_ref))
    copies = [pltpu.make_async_copy(*pair, sems.at[at]) for at, pair in enumerate(pairs)]
    for copy in copies:
        copy.start()
    for copy in copies:
        copy.wait()
    spread_ref[...] = jnp.broadcast_to(rows_ref[...][None], spread_ref.shape)
    pages = columns(pbt_ref[0:1, :], slots)
    numbers = columns(pbt_ref[1:2, :], slots)
    page_count = len_ref.shape[1]
    hit = lax.broadcasted_iota(jnp.int32, (slots, page_count), 1) == pages
    length = jnp.sum(jnp.where(hit, len_ref[...], 0).astype(f32), axis=1, keepdims=True)
    live = length.astype(jnp.int32) - numbers * BROWS
    live_ref[...] = jnp.broadcast_to(jnp.where(pages < 0, 0, live), live_ref.shape)
    page_ref[...] = jnp.broadcast_to(pages, page_ref.shape)
    number_ref[...] = jnp.broadcast_to(numbers, number_ref.shape)


def own_kernel(live_ref, q_ref, p_ref, lse_ref, qt_ref):
    slot_stats(live_ref, q_ref, p_ref, lse_ref, qt_ref, 0)


def stats_kernel(
    ids_ref, live_ref, own_lse_ref, q_ref, p_ref, lse_ref, send_ref, qt_ref
):
    slots, rows = lse_ref.shape
    half = rows // 2
    lse_ref[:, :half] = own_lse_ref[...]
    slot_stats(live_ref, q_ref, p_ref, lse_ref, qt_ref, half)
    pages = ids_ref[:, 0:1]
    first = pages[0:1]
    last = jnp.max(pages, axis=0, keepdims=True)
    values = lse_ref[...]
    head = lse_rows(values, pages == first)
    tail = lse_rows(values, pages == last)
    mine = lax.axis_index("page")
    for peer in range(send_ref.shape[0]):
        up = peer > mine
        send_ref[peer, :, :rows] = jnp.where(up, tail, head)
        send_ref[peer, :, rows:] = jnp.broadcast_to(jnp.where(up, last, first).astype(f32), (1, 128))


def label_signs(pages, lab_ref, rows):
    slots = pages.shape[0]
    queries, page_count = lab_ref.shape
    half = rows // 2
    hit = lax.broadcasted_iota(jnp.int32, (slots, page_count), 1) == pages
    picked = lax.dot_general(
        hit.astype(bf16),
        lab_ref[...].astype(bf16),
        (((1,), (1,)), ((), ())),
        preferred_element_type=f32,
    )
    lane = lax.broadcasted_iota(jnp.int32, (queries, rows), 1)
    question = (lane - jnp.where(lane >= half, half, 0)) // HALF_WORDS
    spread = (question == lax.broadcasted_iota(jnp.int32, (queries, rows), 0)).astype(bf16)
    return 2.0 * jnp.dot(picked.astype(bf16), spread, preferred_element_type=f32) - 1.0


def gradients(value, sign):
    count, rows = value.shape
    half = rows // 2
    same_group = (
        lax.broadcasted_iota(jnp.int32, (CHUNK, CHUNK), 0) // HALF_WORDS
        == lax.broadcasted_iota(jnp.int32, (CHUNK, CHUNK), 1) // HALF_WORDS
    ).astype(bf16)
    totals = []
    for lo in range(0, half, CHUNK):
        total = [
            jnp.dot(term, same_group, preferred_element_type=f32)
            for at in (lo, half + lo)
            for term in three_terms(value[:, at : at + CHUNK])
        ]
        totals.append(total[0] + total[1] + total[2] + (total[3] + total[4] + total[5]))
    totals = totals + totals
    scores = (smoothing_divisor * LN2) * jnp.concatenate(totals, axis=1)
    logits = (logit_scale / QUESTION_WORDS) * scores + logit_bias
    margin = -sign * logits
    small = jnp.exp(-jnp.abs(margin))
    pair = jnp.maximum(margin, 0.0) + jnp.log1p(small)
    sigmoid = jnp.where(margin >= 0.0, 1.0, small) / (1.0 + small)
    return -sign * sigmoid * (logit_scale / QUESTION_WORDS), pair


def inner_kernel(
    pbs_ref, ids_ref, number_ref, live_ref, lab_ref, lse_ref, own_ref, oth_ref, p_ref, page_ref,
    row_ref, sign_ref, loss_ref, acc_ref, weight_ref, qt_ref,
):
    slots, rows = lse_ref.shape
    half = rows // 2
    pages = ids_ref[:, 0:1]
    first = pages[0:1]
    last = jnp.max(pages, axis=0, keepdims=True)
    values = lse_ref[...]
    qt_ref[:, :half] = own_ref[...].T
    qt_ref[:, half:] = oth_ref[...].T
    sign_ref[...] = label_signs(pages, lab_ref, rows)
    for slot in range(slots):
        page_ref[slot : slot + 1, :] = chosen_row(values, pages == pages[slot : slot + 1])
    peak = page_ref[...]
    square = jnp.broadcast_to(pages, (slots, slots))
    diagonal = lax.broadcasted_iota(jnp.int32, (slots, slots), 0) == lax.broadcasted_iota(
        jnp.int32, (slots, slots), 1
    )
    across = jnp.sum(jnp.where(diagonal, square, 0).astype(f32), axis=0, keepdims=True)
    same_page = (square.astype(f32) == across).astype(bf16)
    mass = [
        jnp.dot(same_page, term, preferred_element_type=f32)
        for term in three_terms(jnp.exp2(values - peak))
    ]
    value = jnp.where(pages >= 0, peak + jnp.log2(mass[0] + mass[1] + mass[2]), 0.0)
    row, pair = gradients(value, sign_ref[...])
    inside = (pages != first) & (pages != last)
    counted = inside & (pages >= 0) & (number_ref[:, 0:1] == 0)
    row_ref[...] = row
    weight_ref[...] = jnp.where(inside, row, 1.0)
    page_ref[...] = value
    loss = jnp.sum(jnp.where(counted, pair, 0.0), axis=0, keepdims=True)
    loss_ref[...] = jnp.broadcast_to(jnp.sum(loss, axis=1, keepdims=True), loss_ref.shape)
    acc_ref[...] = jnp.zeros_like(acc_ref)
    head_page = pbs_ref[0, 0]
    tail_page = head_page
    for slot in range(1, slots):
        tail_page = jnp.maximum(tail_page, pbs_ref[0, slot])

    def one(step, carry):
        start = step * GROUP
        blocks = p_ref[pl.ds(pl.multiple_of(start * BROWS, BROWS), GROUP * BROWS), :]
        kinds, turned = [], []
        for part in range(GROUP):
            page = pbs_ref[0, start + part]
            kinds.append(jnp.where(page == head_page, HEAD, jnp.where(page == tail_page, TAIL, INSIDE)))
            turned.append(blocks[part * BROWS : (part + 1) * BROWS].T)
        for lo in range(0, rows, CHUNK):
            product = jnp.dot(blocks, qt_ref[:, lo : lo + CHUNK], preferred_element_type=f32)
            for part in range(GROUP):
                slot = start + part
                at = pl.ds(slot, 1)
                z = masked(product[part * BROWS : (part + 1) * BROWS], live_ref, slot)
                e = jnp.exp2(z * SCALE2 - page_ref[at, lo : lo + CHUNK])
                coupling = (e * weight_ref[at, lo : lo + CHUNK]).astype(bf16)
                acc_ref[kinds[part], :, lo : lo + CHUNK] += jnp.dot(
                    turned[part], coupling, preferred_element_type=f32
                )
        return carry

    steps = slots // GROUP
    lax.fori_loop(0, steps, one, 0, unroll=INNER_UNROLL if rows <= 1024 else 1)


def close_kernel(
    ids_ref, number_ref, sign_ref, page_ref, row_ref, loss_ref, acc_ref, recv_ref, scales_ref, give_ref, lse_ref,
    full_ref, part_ref, got_ref,
):
    slots, rows = page_ref.shape
    peers = recv_ref.shape[0]
    mine = lax.axis_index("page")
    core = mine % 2
    half = rows // 2
    pages = ids_ref[:, 0:1]
    first = pages[0:1]
    last = jnp.max(pages, axis=0, keepdims=True)
    is_first = pages == first
    is_last = pages == last
    alone = first == last

    for peer in range(peers):
        got_ref[peer : peer + 1, :] = recv_ref[peer]
    peer = lax.broadcasted_iota(jnp.int32, (peers, 1), 0)
    got = got_ref[:, :rows]
    crossed = jnp.concatenate([got[:, half:], got[:, :half]], axis=1)
    got = jnp.where(peer % 2 == core, got, crossed)
    ids = got_ref[:, rows : rows + 1]

    def gathered(mask):
        peak = chosen_row(got, mask)
        mass = jnp.sum(jnp.where(mask, jnp.exp2(got - peak), 0.0), axis=0, keepdims=True)
        return peak + jnp.log2(jnp.maximum(mass, 1e-30))

    below = gathered((peer < mine) & (ids == first.astype(f32)))
    above = gathered((peer > mine) & (ids == last.astype(f32)))
    value = page_ref[...]
    head = value[0:1]
    tail = chosen_row(value, is_last)
    head_full = add_lse(head, below)
    head_full = jnp.where(alone, add_lse(head_full, above), head_full)
    tail_full = jnp.where(alone, head_full, add_lse(tail, above))
    both = jnp.concatenate([head_full, tail_full], axis=0)
    sign = sign_ref[...]
    signs = jnp.concatenate([sign[0:1], chosen_row(sign, is_last)], axis=0)
    row, pair = gradients(both, signs)
    starts = number_ref[:, 0:1] == 0
    head_counts = starts[0:1]
    tail_counts = (jnp.max((starts & is_last).astype(jnp.int32), axis=0, keepdims=True) > 0) & jnp.logical_not(alone)
    loss = jnp.sum(
        jnp.where(head_counts, pair[0:1], 0.0) + jnp.where(tail_counts, pair[1:2], 0.0),
        axis=1,
        keepdims=True,
    )
    loss = (loss + loss_ref[...]) * (1.0 / QUESTION_WORDS)
    lse_ref[...] = jnp.where(is_last, tail_full, jnp.where(is_first, head_full, value))
    full_ref[...] = jnp.where(is_last, row[1:2], jnp.where(is_first, row[0:1], row_ref[...]))
    head_scale = row[0:1] * jnp.exp2(head - head_full)
    tail_scale = row[1:2] * jnp.exp2(tail - tail_full)
    scales_ref[0:1, :] = head_scale
    scales_ref[1:2, :] = tail_scale
    combine(acc_ref, scales_ref, give_ref, half)
    part_ref[...] = loss


def combine(acc_ref, scales_ref, out_ref, base):
    for lo in range(0, out_ref.shape[0], CHUNK):
        span = slice(base + lo, base + lo + CHUNK)
        total = (
            acc_ref[INSIDE, :, span]
            + acc_ref[HEAD, :, span] * scales_ref[0:1, span]
            + acc_ref[TAIL, :, span] * scales_ref[1:2, span]
        )
        out_ref[lo : lo + CHUNK, :] = total.T


def keep_kernel(acc_ref, scales_ref, keep_ref):
    combine(acc_ref, scales_ref, keep_ref, 0)


def join_kernel(keep_ref, give_ref, part_ref, row_ref, out_ref, again_ref):
    devices, pairs = out_ref.shape[0], out_ref.shape[1] - 1
    again_ref[...] = row_ref[...]
    high, mid, low = (term.astype(f32) for term in three_terms(part_ref[...]))
    lane = lax.broadcasted_iota(jnp.int32, (1, BROWS), 1)
    loss = jnp.concatenate([jnp.where(lane < LOW_LANES, high, mid), low], axis=0).astype(bf16)
    for device in range(devices):
        base = device * 2 * pairs
        total = keep_ref[base : base + 2 * pairs, :] + give_ref[base : base + 2 * pairs, :]
        for pair in range(pairs):
            out_ref[device, pair] = total[2 * pair : 2 * pair + 2].astype(bf16)
        out_ref[device, pairs] = loss


def patch_kernel(live_ref, lse_ref, row_ref, own_ref, oth_ref, p_ref, out_ref, qt_ref):
    slots, rows = lse_ref.shape
    half = rows // 2
    qt_ref[:, :half] = own_ref[...].T
    qt_ref[:, half:] = oth_ref[...].T

    def one(step, carry):
        start = step * GROUP
        span = pl.ds(pl.multiple_of(start * BROWS, BROWS), GROUP * BROWS)
        blocks = p_ref[span, :]
        total = jnp.zeros((GROUP * BROWS, BROWS), f32)
        for lo in range(0, rows, CHUNK):
            product = jnp.dot(blocks, qt_ref[:, lo : lo + CHUNK], preferred_element_type=f32)
            couplings = []
            for part in range(GROUP):
                at = pl.ds(start + part, 1)
                z = masked(product[part * BROWS : (part + 1) * BROWS], live_ref, start + part)
                weights = jnp.exp2(z * SCALE2 - lse_ref[at, lo : lo + CHUNK])
                couplings.append((row_ref[at, lo : lo + CHUNK] * weights).astype(bf16))
            q_ref, at = (own_ref, lo) if lo < half else (oth_ref, lo - half)
            total = total + jnp.dot(
                jnp.concatenate(couplings, axis=0), q_ref[at : at + CHUNK, :], preferred_element_type=f32
            )
        out_ref[span, :] = total
        return carry

    steps = slots // GROUP
    lax.fori_loop(0, steps, one, 0, unroll=PATCH_UNROLL if rows <= 1024 else 1)


def final_kernel(scale, recv_ref, grad_ref, loss_ref):
    devices, pairs = recv_ref.shape[0], recv_ref.shape[1] - 1
    totals = [jnp.zeros((pairs + 1, 2, BROWS), f32)] * 2
    for device in range(devices):
        totals[device % 2] = totals[device % 2] + recv_ref[device].astype(f32)
    each = HALF_WORDS // 2
    for core in range(2):
        for pair in range(pairs):
            at = pair % each * 2
            grad_ref[pair // each, core, at : at + 2, :] = totals[core][pair]
    both = totals[0][pairs] + totals[1][pairs]
    loss_ref[...] = (both[0:1, :1] + both[0:1, LOW_LANES : LOW_LANES + 1] + both[1:2]) * scale


def call(kernel, name, flops, in_specs, shapes, scratch=(), limit=24):
    return pl.pallas_call(
        kernel,
        in_specs=in_specs,
        out_specs=[VMEM] * len(shapes),
        out_shape=[jax.ShapeDtypeStruct(*shape) for shape in shapes],
        scratch_shapes=[pltpu.VMEM(*shape) if isinstance(shape, tuple) else shape for shape in scratch],
        cost_estimate=pl.CostEstimate(flops=flops, bytes_accessed=0, transcendentals=0),
        compiler_params=pltpu.CompilerParams(vmem_limit_bytes=limit << 20),
        name=name,
    )


def shards(queries, patches, page_blocks, lengths, labels):
    axes = ("grp", "page")
    devices = lax.axis_size(axes)
    peers = lax.axis_size("page")
    slots = page_blocks.shape[0]
    width = patches.shape[1]
    local_rows = queries.reshape(-1, width)
    local = local_rows.shape[0]
    rows = local * devices
    matmul = 2 * rows * patches.shape[0] * width
    half = rows // 2
    table = ((slots, rows), f32)
    half_table = ((slots, half), f32)
    ids = ((slots, BROWS), jnp.int32)
    turned_half = ((width + BROWS, half), bf16)
    limit = 24 if rows <= 1024 else 52
    pbt = page_blocks.T
    questions = local // QUESTION_WORDS
    halves = local_rows.reshape(questions, 2, HALF_WORDS, width).swapaxes(0, 1).reshape(2, local // 2, width)
    inputs = (halves, page_blocks.T, lengths.reshape(1, -1))
    p = patches
    spread, live, pages, numbers = call(
        start_kernel,
        "start",
        4 * matmul,
        [HBM] * 3,
        [((devices // 2, *halves.shape), bf16), ids, ids, ids],
        [
            (halves.shape, bf16),
            (pbt.shape, jnp.int32),
            ((1, lengths.shape[0]), jnp.int32),
            pltpu.SemaphoreType.DMA((3,)),
        ],
    )(*(pltpu.with_memory_space_constraint(x, pltpu.HBM) for x in inputs))
    own = lax.all_to_all(
        spread.reshape(devices, local // 2, width), axes, 0, 0, tiled=True
    ).reshape(half, width)
    pairs = [(i, i ^ 1) for i in range(devices)]
    other = lax.ppermute(own, axes, pairs)
    (own_lse,) = call(
        own_kernel, "own", matmul // 2, [VMEM] * 3, [half_table], [turned_half], limit
    )(live, own, p)
    lse, send = call(
        stats_kernel,
        "stats",
        matmul // 2,
        [VMEM] * 5,
        [table, ((peers, 1, rows + 128), f32)],
        [turned_half],
        limit,
    )(pages, live, own_lse, other, p)
    recv = lax.all_to_all(send, "page", 0, 0, tiled=True)
    page_lse, row, sign, loss, acc = call(
        inner_kernel,
        "inner",
        2 * matmul,
        [SMEM] + [VMEM] * 8,
        [table, table, table, ((1, BROWS), f32), ((3, width, rows), f32)],
        [table, ((width, rows), bf16)],
        limit,
    )(pbt, pages, numbers, live, labels, lse, own, other, p)
    scales, give, full_lse, row_grad, part = call(
        close_kernel,
        "close",
        matmul,
        [VMEM] * 8,
        [
            ((2, rows), f32),
            ((half, width), f32),
            table,
            table,
            ((1, BROWS), f32),
        ],
        [((peers, rows + 128), f32)],
    )(pages, numbers, sign, page_lse, row, loss, acc, recv)
    give = lax.ppermute(give, axes, pairs)
    (keep,) = call(keep_kernel, "keep", matmul // 4, [VMEM] * 2, [((half, width), f32)])(acc, scales)
    parts, row_grad = call(
        join_kernel,
        "join",
        matmul // 8,
        [VMEM] * 4,
        [((devices, local // 4 + 1, 2, width), bf16), table],
    )(keep, give, part, row_grad)
    gathered = lax.all_to_all(parts, axes, 0, 0, tiled=True)
    (patch_grad,) = call(
        patch_kernel, "patch", 2 * matmul, [VMEM] * 6, [(patches.shape, f32)], [((width, rows), bf16)]
    )(live, full_lse, row_grad, own, other, p)
    query_grad, loss = call(
        lambda *refs: final_kernel(QUESTION_WORDS / rows, *refs),
        "final",
        devices * local * width,
        [VMEM],
        [((questions, 2, HALF_WORDS, width), f32), ((1, BROWS), f32)],
    )(gathered)
    return (patch_grad, query_grad.reshape(queries.shape), loss[0, :1])


def solution(mesh):
    placed = (
        P(("grp", "page"), None, None),
        P(("grp", "page"), None),
        P(("grp", "page"), None),
        P(),
        P(),
    )
    return jax.shard_map(
        shards,
        mesh=mesh,
        in_specs=placed,
        out_specs=(P(("grp", "page"), None), P(("grp", "page"), None, None), P()),
        check_vma=False,
    )
```

```python
import jax
import jax.numpy as jnp
from jax import lax
from jax.experimental import pallas as pl
from jax.experimental.pallas import tpu as pltpu
from jax.sharding import PartitionSpec as P

QUESTION_WORDS = 32
HALF_WORDS = QUESTION_WORDS // 2
BROWS = 128

smoothing_divisor = 0.05
logit_scale = 10.0
logit_bias = -4.0
very_low = -1e30
LOG2E = 1.4426950408889634
LN2 = 0.6931471805599453
SCALE2 = LOG2E / smoothing_divisor
CHUNK = 256
LOW_LANES = 64
GROUP = 4
INNER_UNROLL = 4
PATCH_UNROLL = 1
DEAD = -(2.0**93)
INSIDE, HEAD, TAIL = 0, 1, 2

f32 = jnp.float32
bf16 = jnp.bfloat16
VMEM = pl.BlockSpec(memory_space=pltpu.VMEM)
SMEM = pl.BlockSpec(memory_space=pltpu.SMEM)
HBM = pl.BlockSpec(memory_space=pltpu.HBM)


def lse_rows(values, mask):
    peak = jnp.max(jnp.where(mask, values, very_low), axis=0, keepdims=True)
    mass = jnp.sum(jnp.where(mask, jnp.exp2(values - peak), 0.0), axis=0, keepdims=True)
    return peak + jnp.log2(mass)


def add_lse(one, two):
    peak = jnp.maximum(one, two)
    return peak + jnp.log2(jnp.exp2(one - peak) + jnp.exp2(two - peak))


def chosen_row(values, mask):
    return jnp.max(jnp.where(mask, values, very_low), axis=0, keepdims=True)


def three_terms(value):
    high = value.astype(bf16)
    rest = value - high.astype(f32)
    mid = rest.astype(bf16)
    return high, mid, (rest - mid.astype(f32)).astype(bf16)


def block_of(p_ref, slot):
    return p_ref[pl.ds(pl.multiple_of(slot * BROWS, BROWS), BROWS), :]


def masked(z, live_ref, slot):
    rows = lax.broadcasted_iota(jnp.int32, z.shape, 0)
    live = jnp.concatenate([live_ref[pl.ds(slot, 1), :]] * (z.shape[1] // BROWS), axis=1)
    return jnp.where(rows < live, z, DEAD)


def widened(blocks, live_ref, start):
    rows = lax.broadcasted_iota(jnp.int32, (BROWS, BROWS), 0)
    dead = [
        jnp.where(rows < live_ref[pl.ds(start + part, 1), :], 0.0, 1.0).astype(bf16)
        for part in range(blocks.shape[0] // BROWS)
    ]
    return jnp.concatenate([blocks, jnp.concatenate(dead, axis=0)], axis=1)


def marked_queries(qt_ref, q_ref):
    width = q_ref.shape[1]
    qt_ref[:width, :] = q_ref[...].T
    rows = lax.broadcasted_iota(jnp.int32, (BROWS, q_ref.shape[0]), 0)
    qt_ref[width:, :] = jnp.where(rows == 0, DEAD, 0.0).astype(bf16)


def columns(row, count):
    diagonal = lax.broadcasted_iota(jnp.int32, (count, count), 0) == lax.broadcasted_iota(
        jnp.int32, (count, count), 1
    )
    spread = jnp.where(diagonal, jnp.broadcast_to(row, (count, count)), 0).astype(f32)
    return jnp.sum(spread, axis=1, keepdims=True).astype(jnp.int32)


def slot_stats(live_ref, q_ref, p_ref, lse_ref, qt_ref, base):
    slots = lse_ref.shape[0]
    group = slots if q_ref.shape[0] <= 1024 else GROUP
    marked_queries(qt_ref, q_ref)

    def one(step, carry):
        start = step * group
        blocks = p_ref[pl.ds(pl.multiple_of(start * BROWS, BROWS), group * BROWS), :]
        blocks = widened(blocks, live_ref, start)
        for lo in range(0, q_ref.shape[0], CHUNK):
            product = jnp.dot(blocks, qt_ref[:, lo : lo + CHUNK], preferred_element_type=f32)
            for part in range(group):
                slot = start + part
                z = product[part * BROWS : (part + 1) * BROWS]
                top = jnp.max(z, axis=0, keepdims=True)
                mass = jnp.sum(jnp.exp2((z - top) * SCALE2), axis=0, keepdims=True)
                lse_ref[pl.ds(slot, 1), base + lo : base + lo + CHUNK] = top * SCALE2 + jnp.log2(mass)
        return carry

    steps = slots // group
    lax.fori_loop(0, steps, one, 0, unroll=steps if q_ref.shape[0] <= 1024 else 1)


def start_kernel(rows_hbm, spread_ref, rows_ref, sem):
    copy = pltpu.make_async_copy(rows_hbm, rows_ref, sem)
    copy.start()
    copy.wait()
    spread_ref[...] = jnp.broadcast_to(rows_ref[...][None], spread_ref.shape)


def own_kernel(pbt_ref, len_ref, q_ref, p_ref, lse_ref, live_ref, page_ref, number_ref, qt_ref):
    slots = lse_ref.shape[0]
    pages = columns(pbt_ref[0:1, :], slots)
    numbers = columns(pbt_ref[1:2, :], slots)
    page_count = len_ref.shape[1]
    hit = lax.broadcasted_iota(jnp.int32, (slots, page_count), 1) == pages
    length = jnp.sum(jnp.where(hit, len_ref[...], 0).astype(f32), axis=1, keepdims=True)
    live = length.astype(jnp.int32) - numbers * BROWS
    live_ref[...] = jnp.broadcast_to(jnp.where(pages < 0, 0, live), live_ref.shape)
    page_ref[...] = jnp.broadcast_to(pages, page_ref.shape)
    number_ref[...] = jnp.broadcast_to(numbers, number_ref.shape)
    slot_stats(live_ref, q_ref, p_ref, lse_ref, qt_ref, 0)


def stats_kernel(
    ids_ref, live_ref, own_lse_ref, q_ref, p_ref, lse_ref, send_ref, qt_ref
):
    slots, rows = lse_ref.shape
    half = rows // 2
    lse_ref[:, :half] = own_lse_ref[...]
    slot_stats(live_ref, q_ref, p_ref, lse_ref, qt_ref, half)
    pages = ids_ref[:, 0:1]
    first = pages[0:1]
    last = jnp.max(pages, axis=0, keepdims=True)
    values = lse_ref[...]
    head = lse_rows(values, pages == first)
    tail = lse_rows(values, pages == last)
    mine = lax.axis_index("page")
    for peer in range(send_ref.shape[0]):
        up = peer > mine
        send_ref[peer, :, :rows] = jnp.where(up, tail, head)
        send_ref[peer, :, rows:] = jnp.broadcast_to(jnp.where(up, last, first).astype(f32), (1, 128))


def label_signs(pages, lab_ref, rows):
    slots = pages.shape[0]
    queries, page_count = lab_ref.shape
    half = rows // 2
    hit = lax.broadcasted_iota(jnp.int32, (slots, page_count), 1) == pages
    picked = lax.dot_general(
        hit.astype(bf16),
        lab_ref[...].astype(bf16),
        (((1,), (1,)), ((), ())),
        preferred_element_type=f32,
    )
    lane = lax.broadcasted_iota(jnp.int32, (queries, rows), 1)
    question = (lane - jnp.where(lane >= half, half, 0)) // HALF_WORDS
    spread = (question == lax.broadcasted_iota(jnp.int32, (queries, rows), 0)).astype(bf16)
    return 2.0 * jnp.dot(picked.astype(bf16), spread, preferred_element_type=f32) - 1.0


def gradients(value, sign):
    count, rows = value.shape
    half = rows // 2
    same_group = (
        lax.broadcasted_iota(jnp.int32, (CHUNK, CHUNK), 0) // HALF_WORDS
        == lax.broadcasted_iota(jnp.int32, (CHUNK, CHUNK), 1) // HALF_WORDS
    ).astype(bf16)
    totals = []
    for lo in range(0, half, CHUNK):
        total = [
            jnp.dot(term, same_group, preferred_element_type=f32)
            for at in (lo, half + lo)
            for term in three_terms(value[:, at : at + CHUNK])
        ]
        totals.append(total[0] + total[1] + total[2] + (total[3] + total[4] + total[5]))
    totals = totals + totals
    scores = (smoothing_divisor * LN2) * jnp.concatenate(totals, axis=1)
    logits = (logit_scale / QUESTION_WORDS) * scores + logit_bias
    margin = -sign * logits
    small = jnp.exp(-jnp.abs(margin))
    pair = jnp.maximum(margin, 0.0) + jnp.log1p(small)
    sigmoid = jnp.where(margin >= 0.0, 1.0, small) / (1.0 + small)
    return -sign * sigmoid * (logit_scale / QUESTION_WORDS), pair


def inner_kernel(
    pbs_ref, ids_ref, number_ref, live_ref, lab_ref, lse_ref, own_ref, oth_ref, p_ref, page_ref,
    row_ref, sign_ref, loss_ref, acc_ref, weight_ref, qt_ref,
):
    slots, rows = lse_ref.shape
    half = rows // 2
    pages = ids_ref[:, 0:1]
    first = pages[0:1]
    last = jnp.max(pages, axis=0, keepdims=True)
    values = lse_ref[...]
    qt_ref[:, :half] = own_ref[...].T
    qt_ref[:, half:] = oth_ref[...].T
    sign_ref[...] = label_signs(pages, lab_ref, rows)
    for slot in range(slots):
        page_ref[slot : slot + 1, :] = chosen_row(values, pages == pages[slot : slot + 1])
    peak = page_ref[...]
    square = jnp.broadcast_to(pages, (slots, slots))
    diagonal = lax.broadcasted_iota(jnp.int32, (slots, slots), 0) == lax.broadcasted_iota(
        jnp.int32, (slots, slots), 1
    )
    across = jnp.sum(jnp.where(diagonal, square, 0).astype(f32), axis=0, keepdims=True)
    same_page = (square.astype(f32) == across).astype(bf16)
    mass = [
        jnp.dot(same_page, term, preferred_element_type=f32)
        for term in three_terms(jnp.exp2(values - peak))
    ]
    value = jnp.where(pages >= 0, peak + jnp.log2(mass[0] + mass[1] + mass[2]), 0.0)
    row, pair = gradients(value, sign_ref[...])
    inside = (pages != first) & (pages != last)
    counted = inside & (pages >= 0) & (number_ref[:, 0:1] == 0)
    row_ref[...] = row
    weight_ref[...] = jnp.where(inside, row, 1.0)
    page_ref[...] = value
    loss = jnp.sum(jnp.where(counted, pair, 0.0), axis=0, keepdims=True)
    loss_ref[...] = jnp.broadcast_to(jnp.sum(loss, axis=1, keepdims=True), loss_ref.shape)
    acc_ref[...] = jnp.zeros_like(acc_ref)
    head_page = pbs_ref[0, 0]
    tail_page = head_page
    for slot in range(1, slots):
        tail_page = jnp.maximum(tail_page, pbs_ref[0, slot])

    def one(step, carry):
        start = step * GROUP
        blocks = p_ref[pl.ds(pl.multiple_of(start * BROWS, BROWS), GROUP * BROWS), :]
        kinds, turned = [], []
        for part in range(GROUP):
            page = pbs_ref[0, start + part]
            kinds.append(jnp.where(page == head_page, HEAD, jnp.where(page == tail_page, TAIL, INSIDE)))
            turned.append(blocks[part * BROWS : (part + 1) * BROWS].T)
        for lo in range(0, rows, CHUNK):
            product = jnp.dot(blocks, qt_ref[:, lo : lo + CHUNK], preferred_element_type=f32)
            for part in range(GROUP):
                slot = start + part
                at = pl.ds(slot, 1)
                z = masked(product[part * BROWS : (part + 1) * BROWS], live_ref, slot)
                e = jnp.exp2(z * SCALE2 - page_ref[at, lo : lo + CHUNK])
                coupling = (e * weight_ref[at, lo : lo + CHUNK]).astype(bf16)
                acc_ref[kinds[part], :, lo : lo + CHUNK] += jnp.dot(
                    turned[part], coupling, preferred_element_type=f32
                )
        return carry

    steps = slots // GROUP
    lax.fori_loop(0, steps, one, 0, unroll=INNER_UNROLL if rows <= 1024 else 1)


def close_kernel(
    ids_ref, number_ref, sign_ref, page_ref, loss_ref, acc_ref, recv_ref, scales_ref, give_ref, both_ref, part_ref,
    got_ref,
):
    slots, rows = page_ref.shape
    peers = recv_ref.shape[0]
    mine = lax.axis_index("page")
    core = mine % 2
    half = rows // 2
    pages = ids_ref[:, 0:1]
    first = pages[0:1]
    last = jnp.max(pages, axis=0, keepdims=True)
    is_last = pages == last
    alone = first == last

    for peer in range(peers):
        got_ref[peer : peer + 1, :] = recv_ref[peer]
    peer = lax.broadcasted_iota(jnp.int32, (peers, 1), 0)
    got = got_ref[:, :rows]
    crossed = jnp.concatenate([got[:, half:], got[:, :half]], axis=1)
    got = jnp.where(peer % 2 == core, got, crossed)
    ids = got_ref[:, rows : rows + 1]

    def gathered(mask):
        peak = chosen_row(got, mask)
        mass = jnp.sum(jnp.where(mask, jnp.exp2(got - peak), 0.0), axis=0, keepdims=True)
        return peak + jnp.log2(jnp.maximum(mass, 1e-30))

    below = gathered((peer < mine) & (ids == first.astype(f32)))
    above = gathered((peer > mine) & (ids == last.astype(f32)))
    value = page_ref[...]
    head = value[0:1]
    tail = chosen_row(value, is_last)
    head_full = add_lse(head, below)
    head_full = jnp.where(alone, add_lse(head_full, above), head_full)
    tail_full = jnp.where(alone, head_full, add_lse(tail, above))
    both = jnp.concatenate([head_full, tail_full], axis=0)
    sign = sign_ref[...]
    signs = jnp.concatenate([sign[0:1], chosen_row(sign, is_last)], axis=0)
    row, pair = gradients(both, signs)
    starts = number_ref[:, 0:1] == 0
    head_counts = starts[0:1]
    tail_counts = (jnp.max((starts & is_last).astype(jnp.int32), axis=0, keepdims=True) > 0) & jnp.logical_not(alone)
    loss = jnp.sum(
        jnp.where(head_counts, pair[0:1], 0.0) + jnp.where(tail_counts, pair[1:2], 0.0),
        axis=1,
        keepdims=True,
    )
    loss = (loss + loss_ref[...]) * (1.0 / QUESTION_WORDS)
    both_ref[0:2, :] = both
    both_ref[2:4, :] = row
    head_scale = row[0:1] * jnp.exp2(head - head_full)
    tail_scale = row[1:2] * jnp.exp2(tail - tail_full)
    scales_ref[0:1, :] = head_scale
    scales_ref[1:2, :] = tail_scale
    combine(acc_ref, scales_ref, give_ref, half)
    part_ref[...] = loss


def combine(acc_ref, scales_ref, out_ref, base):
    for lo in range(0, out_ref.shape[0], CHUNK):
        span = slice(base + lo, base + lo + CHUNK)
        total = (
            acc_ref[INSIDE, :, span]
            + acc_ref[HEAD, :, span] * scales_ref[0:1, span]
            + acc_ref[TAIL, :, span] * scales_ref[1:2, span]
        )
        out_ref[lo : lo + CHUNK, :] = total.T


def keep_kernel(ids_ref, page_ref, row_ref, both_ref, acc_ref, scales_ref, keep_ref, lse_ref, full_ref):
    pages = ids_ref[:, 0:1]
    is_first = pages == pages[0:1]
    is_last = pages == jnp.max(pages, axis=0, keepdims=True)

    def filled(at, values):
        head, tail = both_ref[at : at + 1, :], both_ref[at + 1 : at + 2, :]
        return jnp.where(is_last, tail, jnp.where(is_first, head, values))

    lse_ref[...] = filled(0, page_ref[...])
    full_ref[...] = filled(2, row_ref[...])
    combine(acc_ref, scales_ref, keep_ref, 0)


def join_kernel(keep_ref, give_ref, part_ref, row_ref, out_ref, again_ref):
    devices, pairs = out_ref.shape[0], out_ref.shape[1] - 1
    again_ref[...] = row_ref[...]
    high, mid, low = (term.astype(f32) for term in three_terms(part_ref[...]))
    lane = lax.broadcasted_iota(jnp.int32, (1, BROWS), 1)
    loss = jnp.concatenate([jnp.where(lane < LOW_LANES, high, mid), low], axis=0).astype(bf16)
    for device in range(devices):
        base = device * 2 * pairs
        total = keep_ref[base : base + 2 * pairs, :] + give_ref[base : base + 2 * pairs, :]
        for pair in range(pairs):
            out_ref[device, pair] = total[2 * pair : 2 * pair + 2].astype(bf16)
        out_ref[device, pairs] = loss


def patch_kernel(live_ref, lse_ref, row_ref, own_ref, oth_ref, p_ref, out_ref, qt_ref):
    slots, rows = lse_ref.shape
    half = rows // 2
    qt_ref[:, :half] = own_ref[...].T
    qt_ref[:, half:] = oth_ref[...].T

    def one(step, carry):
        start = step * GROUP
        span = pl.ds(pl.multiple_of(start * BROWS, BROWS), GROUP * BROWS)
        blocks = p_ref[span, :]
        total = jnp.zeros((GROUP * BROWS, BROWS), f32)
        for lo in range(0, rows, CHUNK):
            product = jnp.dot(blocks, qt_ref[:, lo : lo + CHUNK], preferred_element_type=f32)
            couplings = []
            for part in range(GROUP):
                at = pl.ds(start + part, 1)
                z = masked(product[part * BROWS : (part + 1) * BROWS], live_ref, start + part)
                weights = jnp.exp2(z * SCALE2 - lse_ref[at, lo : lo + CHUNK])
                couplings.append((row_ref[at, lo : lo + CHUNK] * weights).astype(bf16))
            q_ref, at = (own_ref, lo) if lo < half else (oth_ref, lo - half)
            total = total + jnp.dot(
                jnp.concatenate(couplings, axis=0), q_ref[at : at + CHUNK, :], preferred_element_type=f32
            )
        out_ref[span, :] = total
        return carry

    steps = slots // GROUP
    lax.fori_loop(0, steps, one, 0, unroll=PATCH_UNROLL if rows <= 1024 else 1)


def final_kernel(scale, recv_ref, grad_ref, loss_ref):
    devices, pairs = recv_ref.shape[0], recv_ref.shape[1] - 1
    totals = [jnp.zeros((pairs + 1, 2, BROWS), f32)] * 2
    for device in range(devices):
        totals[device % 2] = totals[device % 2] + recv_ref[device].astype(f32)
    each = HALF_WORDS // 2
    for core in range(2):
        for pair in range(pairs):
            at = pair % each * 2
            grad_ref[pair // each, core, at : at + 2, :] = totals[core][pair]
    both = totals[0][pairs] + totals[1][pairs]
    loss_ref[...] = (both[0:1, :1] + both[0:1, LOW_LANES : LOW_LANES + 1] + both[1:2]) * scale


def call(kernel, name, flops, in_specs, shapes, scratch=(), limit=24):
    return pl.pallas_call(
        kernel,
        in_specs=in_specs,
        out_specs=[VMEM] * len(shapes),
        out_shape=[jax.ShapeDtypeStruct(*shape) for shape in shapes],
        scratch_shapes=[pltpu.VMEM(*shape) if isinstance(shape, tuple) else shape for shape in scratch],
        cost_estimate=pl.CostEstimate(flops=flops, bytes_accessed=0, transcendentals=0),
        compiler_params=pltpu.CompilerParams(vmem_limit_bytes=limit << 20),
        name=name,
    )


def shards(queries, patches, page_blocks, lengths, labels):
    axes = ("grp", "page")
    devices = lax.axis_size(axes)
    peers = lax.axis_size("page")
    slots = page_blocks.shape[0]
    width = patches.shape[1]
    local_rows = queries.reshape(-1, width)
    local = local_rows.shape[0]
    rows = local * devices
    matmul = 2 * rows * patches.shape[0] * width
    half = rows // 2
    table = ((slots, rows), f32)
    half_table = ((slots, half), f32)
    ids = ((slots, BROWS), jnp.int32)
    turned_half = ((width + BROWS, half), bf16)
    limit = 24 if rows <= 1024 else 52
    pbt = page_blocks.T
    questions = local // QUESTION_WORDS
    halves = local_rows.reshape(questions, 2, HALF_WORDS, width).swapaxes(0, 1).reshape(2, local // 2, width)
    p = patches
    (spread,) = call(
        start_kernel,
        "start",
        4 * matmul,
        [HBM],
        [((devices // 2, *halves.shape), bf16)],
        [(halves.shape, bf16), pltpu.SemaphoreType.DMA],
    )(pltpu.with_memory_space_constraint(halves, pltpu.HBM))
    own = lax.all_to_all(
        spread.reshape(devices, local // 2, width), axes, 0, 0, tiled=True
    ).reshape(half, width)
    pairs = [(i, i ^ 1) for i in range(devices)]
    other = lax.ppermute(own, axes, pairs)
    own_lse, live, pages, numbers = call(
        own_kernel, "own", matmul // 2, [VMEM] * 4, [half_table, ids, ids, ids], [turned_half], limit
    )(pbt, lengths.reshape(1, -1), own, p)
    lse, send = call(
        stats_kernel,
        "stats",
        matmul // 2,
        [VMEM] * 5,
        [table, ((peers, 1, rows + 128), f32)],
        [turned_half],
        limit,
    )(pages, live, own_lse, other, p)
    recv = lax.all_to_all(send, "page", 0, 0, tiled=True)
    page_lse, row, sign, loss, acc = call(
        inner_kernel,
        "inner",
        2 * matmul,
        [SMEM] + [VMEM] * 8,
        [table, table, table, ((1, BROWS), f32), ((3, width, rows), f32)],
        [table, ((width, rows), bf16)],
        limit,
    )(pbt, pages, numbers, live, labels, lse, own, other, p)
    scales, give, both, part = call(
        close_kernel,
        "close",
        matmul,
        [VMEM] * 7,
        [((2, rows), f32), ((half, width), f32), ((4, rows), f32), ((1, BROWS), f32)],
        [((peers, rows + 128), f32)],
    )(pages, numbers, sign, page_lse, loss, acc, recv)
    give = lax.ppermute(give, axes, pairs)
    keep, full_lse, row_grad = call(
        keep_kernel, "keep", matmul // 4, [VMEM] * 6, [((half, width), f32), table, table]
    )(pages, page_lse, row, both, acc, scales)
    parts, row_grad = call(
        join_kernel,
        "join",
        matmul // 8,
        [VMEM] * 4,
        [((devices, local // 4 + 1, 2, width), bf16), table],
    )(keep, give, part, row_grad)
    gathered = lax.all_to_all(parts, axes, 0, 0, tiled=True)
    (patch_grad,) = call(
        patch_kernel, "patch", 2 * matmul, [VMEM] * 6, [(patches.shape, f32)], [((width, rows), bf16)]
    )(live, full_lse, row_grad, own, other, p)
    query_grad, loss = call(
        lambda *refs: final_kernel(QUESTION_WORDS / rows, *refs),
        "final",
        devices * local * width,
        [VMEM],
        [((questions, 2, HALF_WORDS, width), f32), ((1, BROWS), f32)],
    )(gathered)
    return (patch_grad, query_grad.reshape(queries.shape), loss[0, :1])


def solution(mesh):
    placed = (
        P(("grp", "page"), None, None),
        P(("grp", "page"), None),
        P(("grp", "page"), None),
        P(),
        P(),
    )
    return jax.shard_map(
        shards,
        mesh=mesh,
        in_specs=placed,
        out_specs=(P(("grp", "page"), None), P(("grp", "page"), None, None), P()),
        check_vma=False,
    )
```
